32 devices in a mesh: row: 4 (over x, core), col: 8 (over z, y).
Axes of the slice: x: 2, y: 2, z: 4, core: 2. Of those that a mesh axis runs over, the one named last changes fastest.
Arguments:
- panel: bfloat16 [32768, 512], P('row', 'col'), may hold values from -0.03125 to 0.03125
- pheno: bfloat16 [32768, 2048], P('row', 'col'), may hold values from -48 to 48
- kin_values: float32 [512], replicated, may hold values from 0.1 to 10
- trait_values: float32 [128], replicated, may hold values from 0.1 to 10
- trait_basis: float32 [128, 128], replicated, may hold values from -0.5 to 0.5
Outputs:
- coeffs: float32 [512, 2048], P('row', 'col')
- genetic: bfloat16 [32768, 2048], P('row', 'col')
The draws below stay inside these ranges and needn't reach their ends.
All inputs are finite; a program needn't handle non-finite values.
Results may differ from the reference program's by a relative error of at most 0.0049.
Values may be sent and summed in bfloat16 or wider, within the bound.
A program may use at most 64 MiB of HBM per device.

```python
import math
import jax
import jax.numpy as jnp
from jax import lax

PANEL = 512
TRAITS = 128
NIND = 32768
SETS = 16


def block_levels(key, dims, pieces, smallest, high):
    gain = 1.0
    for dim, blocks in pieces:
        draws = jax.random.uniform(jax.random.fold_in(jax.random.fold_in(key, 6), dim), (blocks,), jnp.float32, smallest / len(pieces), high / len(pieces))
        gain = gain * jnp.repeat(jnp.exp(draws), dims[dim] // blocks).reshape((-1,) + (1,) * (len(dims) - 1 - dim))
    return gain


def gaussian(rng, shape, width, bound, cuts=(), kind=jnp.bfloat16):
    values = jax.random.normal(rng, shape, jnp.float32) * width
    if len(cuts) > 0:
        values = block_levels(rng, shape, cuts, -0.22, 0.18) * values
    return jnp.clip(values, min=-bound, max=bound).astype(kind)


def setup_inputs(seed: int = 0) -> dict:
    key_list = jax.random.split(jax.random.key(seed), 6)
    panel = gaussian(key_list[0], (NIND, PANEL), NIND ** -0.5, 0.03125, ((0, 4), (1, 8)))
    pheno = gaussian(key_list[1], (NIND, TRAITS * SETS), 8.0, 48.0, ((0, 4), (1, 8)))
    kin_values = jnp.clip(jnp.exp(jax.random.uniform(key_list[2], (PANEL,), jnp.float32, math.log(0.1), math.log(10.0))), 0.1, 10.0)
    trait_values = jnp.clip(jnp.exp(jax.random.uniform(key_list[3], (TRAITS,), jnp.float32, math.log(0.1), math.log(10.0))), 0.1, 10.0)
    trait_basis = gaussian(key_list[4], (TRAITS, TRAITS), TRAITS ** -0.5, 0.5, (), jnp.float32)
    return {"panel": panel, "pheno": pheno, "kin_values": kin_values, "trait_values": trait_values, "trait_basis": trait_basis}


def reference(panel, pheno, kin_values, trait_values, trait_basis):
    projected = jnp.dot(panel.T, pheno, preferred_element_type=jnp.float32)
    layered = projected.reshape(PANEL, TRAITS, SETS)
    rotated = jnp.einsum("pts,tj->psj", layered, trait_basis, precision=lax.Precision.HIGHEST)
    product = kin_values[:, None] * trait_values[None, :]
    scaled = rotated * (product / (product + 1.0))[:, None, :]
    unrotated = jnp.einsum("psj,tj->pts", scaled, trait_basis, precision=lax.Precision.HIGHEST)
    coeffs = unrotated.reshape(PANEL, TRAITS * SETS)
    genetic = jnp.dot(panel, coeffs.astype(jnp.bfloat16), preferred_element_type=jnp.float32)
    return coeffs, genetic.astype(jnp.bfloat16)
```

```python
import functools

import jax
import jax.numpy as jnp
from jax import lax
from jax.experimental import pallas as pl
from jax.experimental.pallas import tpu as pltpu
from jax.sharding import PartitionSpec as P

LANES = 128
PIECES = 4
TILES = 16
MESH = pl.DeviceIdType.MESH
HIGH = lax.Precision.HIGHEST


def gather_rotate(
    rows, cols, q, pheno, basis_in, kin_in, trait_in,
    w_out, c_out,
    basis, kin, trait, g, ph, acc, part_f, part, rparts, sb, rb, ob, crow, ct,
    load_sem, send_sem, recv_sem, rs_send, rs_recv, a1_send, a1_recv, a2_send, a2_recv, ag_send, ag_recv,
):
    me_r, me_c = lax.axis_index("row"), lax.axis_index("col")
    lines = cols // 2
    z, y = me_c // 2, lax.rem(me_c, 2)
    other = me_c + 1 - 2 * y
    width, people = q.shape
    piece = people // PIECES
    columns = pheno.shape[1]
    traits = basis.shape[0]
    sets = columns * cols // traits
    t_here = traits // cols

    own_load = pltpu.make_async_copy(q, g.at[me_c], load_sem.at[0])
    own_load.start()
    ph_load = pltpu.make_async_copy(pheno, ph, load_sem.at[1])
    ph_load.start()
    small = [
        pltpu.make_async_copy(a, b, load_sem.at[2 + i])
        for i, (a, b) in enumerate(((basis_in, basis), (kin_in, kin), (trait_in, trait)))
    ]
    for copy in small:
        copy.start()

    barrier = pltpu.get_barrier_semaphore()
    for d in range(1, cols):
        pl.semaphore_signal(barrier, inc=1, device_id=(me_r, lax.rem(me_c + d, cols)), device_id_type=MESH)
    for d in range(1, rows):
        pl.semaphore_signal(barrier, inc=1, device_id=(lax.rem(me_r + d, rows), me_c), device_id_type=MESH)
    pl.semaphore_wait(barrier, cols + rows - 2)

    def hop(way, block, j):
        target = (jnp.minimum(me_c + 2, cols - 2 + y), jnp.maximum(me_c - 2, y), other)[way]
        here = g.at[block, :, pl.ds(j * piece, piece)]
        return pltpu.make_async_remote_copy(
            src_ref=here, dst_ref=here,
            send_sem=send_sem.at[way, block, j], recv_sem=recv_sem.at[block, j],
            device_id=(me_r, target), device_id_type=MESH,
        )

    def arrived(block, j):
        hop(2, block, j).wait_recv()

    up, down = z < lines - 1, z > 0
    late = PIECES // 2

    def line_sends(block, j, act):
        @pl.when(up)
        def _():
            act(hop(0, block, j))

        @pl.when(down)
        def _():
            act(hop(1, block, j))

    own_load.wait()
    for j in range(PIECES):
        line_sends(me_c, j, lambda h: h.start())
        hop(2, me_c, j).start()

    acc[...] = jnp.zeros_like(acc)
    ph_load.wait()

    def process(pair, j):
        arrived(2 * pair + 1 - y, j)
        lanes = pl.ds(pl.multiple_of(pair * LANES, LANES), LANES)
        at = pl.ds(j * piece, piece)
        lhs = jnp.concatenate([g[2 * pair, :, at], g[2 * pair + 1, :, at]], axis=0)
        acc[pair] += jnp.dot(lhs, ph[at, :], preferred_element_type=jnp.float32)
        w_out[at, lanes] = lhs.T

    def by_set(s):
        return part_f[pl.ds(s, t_here, stride=sets), :]

    def finish_pair(pair):
        @pl.when(pair != me_r)
        def _():
            part_f[...] = acc[pair].T
            for s in range(sets):
                part[pair, s * t_here:(s + 1) * t_here, :] = by_set(s).astype(jnp.bfloat16)
            reduce_copy(pair).start()

    def reduce_copy(pair):
        return pltpu.make_async_remote_copy(
            src_ref=part.at[pair], dst_ref=rparts.at[me_r],
            send_sem=rs_send.at[pair], recv_sem=rs_recv.at[me_r],
            device_id=(pair, me_c), device_id_type=MESH,
        )

    def around(s, fn):
        if s == 0:
            fn(z)
            return

        def side(i, _):
            pair = z - s + 2 * s * i

            @pl.when(jnp.logical_and(pair >= 0, pair < lines))
            def _():
                fn(pair)

            return 0

        lax.fori_loop(0, 2, side, 0)

    order = [(0, j) for j in range(PIECES)] + [(1, j) for j in range(late)]
    order += [(s, j) for s in range(2, lines) for j in range(PIECES)]
    tail = [(1, j) for j in range(late, PIECES)]
    done = 0

    def handle(s, j):
        around(s, lambda pair: process(pair, j))
        if j == PIECES - 1:
            around(s, finish_pair)

    for s in range(1, lines):
        for j in range(PIECES):
            skip = s == 1 and j >= late

            @pl.when(z - s >= 0)
            def _():
                b = me_c - 2 * s
                arrived(b, j)

                @pl.when(up)
                def _():
                    hop(0, b, j).start()

                if not skip:
                    hop(2, b, j).start()

            @pl.when(z + s < lines)
            def _():
                b = me_c + 2 * s
                arrived(b, j)

                @pl.when(down)
                def _():
                    hop(1, b, j).start()

                if not skip:
                    hop(2, b, j).start()

            if (s, j) != (1, 0):
                handle(*order[done])
                done += 1
    for j in range(late, PIECES):
        line_sends(other, j, lambda h: h.start())
    rest = order[done:]
    while rest or tail:
        if rest and len(rest) > len(tail):
            handle(*rest.pop(0))
        else:
            handle(*tail.pop(0))

    part_f[...] = acc[me_r].T
    total = jnp.concatenate([by_set(s) for s in range(sets)], axis=0)
    for d in range(1, rows):
        src = lax.rem(me_r + d, rows)
        pltpu.make_async_remote_copy(
            src_ref=part.at[src], dst_ref=rparts.at[src], send_sem=rs_send.at[src], recv_sem=rs_recv.at[src],
            device_id=(src, me_c), device_id_type=MESH,
        ).wait_recv()
        total = total + rparts[src].astype(jnp.float32)
    sb[...] = total.astype(jnp.bfloat16).reshape(sb.shape)

    def trade1(peer, slot):
        return pltpu.make_async_remote_copy(
            src_ref=sb.at[peer], dst_ref=rb.at[slot], send_sem=a1_send.at[peer], recv_sem=a1_recv.at[slot],
            device_id=(me_r, peer), device_id_type=MESH,
        )

    def trade2(peer, slot):
        return pltpu.make_async_remote_copy(
            src_ref=ob.at[peer], dst_ref=crow.at[me_r, slot], send_sem=a2_send.at[peer], recv_sem=a2_recv.at[slot],
            device_id=(me_r, peer), device_id_type=MESH,
        )

    def share(peer, slot):
        return pltpu.make_async_remote_copy(
            src_ref=crow.at[me_r], dst_ref=crow.at[slot], send_sem=ag_send.at[peer], recv_sem=ag_recv.at[slot],
            device_id=(peer, me_c), device_id_type=MESH,
        )

    col_peers = [lax.rem(me_c + d, cols) for d in range(1, cols)]
    row_peers = [lax.rem(me_r + d, rows) for d in range(1, rows)]
    for p in col_peers:
        trade1(p, me_c).start()
    rb[me_c] = sb[me_c]
    for copy in small:
        copy.wait()
    product = kin[pl.ds(me_r, 1), :] * jnp.broadcast_to(trait[...], (LANES, traits)).T
    weight = product / (product + 1.0)
    for p in col_peers:
        trade1(p, p).wait_recv()
    s_here = sets // cols
    got = jnp.concatenate(
        [rb[:, s * t_here:(s + 1) * t_here, :].astype(jnp.float32).reshape(traits, LANES) for s in range(s_here)], axis=1
    )
    rotated = jnp.dot(basis[...].T, got, precision=HIGH, preferred_element_type=jnp.float32)
    scaled = rotated * jnp.concatenate([weight] * s_here, axis=1)
    back = jnp.dot(basis[...], scaled, precision=HIGH, preferred_element_type=jnp.float32)
    for s in range(s_here):
        ob[:, s * t_here:(s + 1) * t_here, :] = (
            back[:, s * LANES:(s + 1) * LANES].reshape(cols, t_here, LANES).astype(jnp.bfloat16)
        )
    for p in col_peers:
        trade2(p, me_c).start()
    crow[me_r, me_c] = ob[me_c]
    for p in col_peers:
        trade2(p, p).wait_recv()
    for p in row_peers:
        share(p, me_r).start()

    def place(r):
        for s in range(sets):
            part_s = crow[r, s // s_here, (s % s_here) * t_here:(s % s_here + 1) * t_here, :]
            ct[pl.ds(s, t_here, stride=sets), :] = part_s.astype(jnp.float32)
        c_out[pl.ds(pl.multiple_of(r * LANES, LANES), LANES), :] = ct[...].T.astype(jnp.bfloat16)

    place(me_r)
    for p in row_peers:
        share(p, p).wait_recv()
        place(p)

    for j in range(PIECES):
        line_sends(me_c, j, lambda h: h.wait_send())
        hop(2, me_c, j).wait_send()
        if j >= late:
            line_sends(other, j, lambda h: h.wait_send())
        for s in range(1, lines):
            skip = s == 1 and j >= late

            @pl.when(z - s >= 0)
            def _():
                @pl.when(up)
                def _():
                    hop(0, me_c - 2 * s, j).wait_send()

                if not skip:
                    hop(2, me_c - 2 * s, j).wait_send()

            @pl.when(z + s < lines)
            def _():
                @pl.when(down)
                def _():
                    hop(1, me_c + 2 * s, j).wait_send()

                if not skip:
                    hop(2, me_c + 2 * s, j).wait_send()

    for p in row_peers:
        reduce_copy(p).wait_send()
        share(p, me_r).wait_send()
    for p in col_peers:
        trade1(p, me_c).wait_send()
        trade2(p, me_c).wait_send()


def predict(w, c, gen_out, coeffs, held, gen_sem):
    share = coeffs.shape[0]
    size = w.shape[0] // TILES

    def emit(i):
        at = pl.ds(pl.multiple_of(i * size, size), size)
        return pltpu.make_async_copy(held.at[at], gen_out.at[at], gen_sem.at[i])

    def step(i, _):
        at = pl.ds(pl.multiple_of(i * size, size), size)
        held[at, :] = jnp.dot(w[at, :], c[...], preferred_element_type=jnp.float32).astype(jnp.bfloat16)
        emit(i).start()
        return 0

    lax.fori_loop(0, TILES, step, 0)
    mine = pl.ds(pl.multiple_of(lax.axis_index("row") * share, share), share)
    coeffs[...] = c[mine, :].astype(jnp.float32)

    def finish(i, _):
        emit(i).wait()
        return 0

    lax.fori_loop(0, TILES, finish, 0)


def fused(panel, pheno, kin_values, trait_values, trait_basis):
    rows, cols = lax.axis_size("row"), lax.axis_size("col")
    ind, columns = pheno.shape
    traits = trait_basis.shape[0]
    sets = columns * cols // traits
    share = kin_values.shape[0] // rows
    bf, f32 = jnp.bfloat16, jnp.float32
    hbm = pl.BlockSpec(memory_space=pltpu.HBM)
    vmem = pl.BlockSpec(memory_space=pltpu.VMEM)
    lot = columns // cols
    dma = pltpu.SemaphoreType.DMA
    given = (panel.T, pheno, trait_basis, kin_values.reshape(rows, share), trait_values[None, :])
    whole, low = pl.pallas_call(
        functools.partial(gather_rotate, rows, cols),
        out_shape=(
            pltpu.VMEM((ind, rows * share), bf),
            pltpu.VMEM((rows * share, columns), bf),
        ),
        in_specs=[hbm] * 5,
        out_specs=(vmem, vmem),
        scratch_shapes=[
            pltpu.VMEM((traits, traits), f32),
            pltpu.VMEM((rows, share), f32),
            pltpu.VMEM((1, traits), f32),
            pltpu.VMEM((cols, panel.shape[1], ind), bf),
            pltpu.VMEM((ind, columns), bf),
            pltpu.VMEM((cols // 2, share, columns), f32),
            pltpu.VMEM((columns, LANES), f32),
            pltpu.VMEM((rows, columns, LANES), bf),
            pltpu.VMEM((rows, columns, LANES), bf),
            pltpu.VMEM((cols, lot, LANES), bf),
            pltpu.VMEM((cols, lot, LANES), bf),
            pltpu.VMEM((cols, lot, LANES), bf),
            pltpu.VMEM((rows, cols, lot, LANES), bf),
            pltpu.VMEM((columns, LANES), f32),
            dma((5,)), dma((3, cols, PIECES)), dma((cols, PIECES)),
            dma((rows,)), dma((rows,)), dma((cols,)), dma((cols,)), dma((cols,)), dma((cols,)),
            dma((rows,)), dma((rows,)),
        ],
        compiler_params=pltpu.CompilerParams(
            collective_id=0, has_side_effects=True, vmem_limit_bytes=30 * 1024 * 1024
        ),
    )(*(pltpu.with_memory_space_constraint(a, pltpu.HBM) for a in given))
    genetic, coeffs = pl.pallas_call(
        predict,
        out_shape=(
            jax.ShapeDtypeStruct((ind, columns), bf),
            jax.ShapeDtypeStruct((share, columns), f32),
        ),
        in_specs=[vmem] * 2,
        out_specs=(hbm, vmem),
        scratch_shapes=[pltpu.VMEM((ind, columns), bf), dma((TILES,))],
        compiler_params=pltpu.CompilerParams(vmem_limit_bytes=20 * 1024 * 1024),
    )(whole, low)
    return coeffs, genetic


def local(panel, pheno, kin_values, trait_values, trait_basis):
    rows, cols = lax.axis_size("row"), lax.axis_size("col")
    eigen = kin_values.shape[0]
    if 2 * panel.shape[1] == LANES and eigen // rows == LANES and trait_basis.shape[0] // cols == 16:
        return fused(panel, pheno, kin_values, trait_values, trait_basis)
    return plain(panel, pheno, kin_values, trait_values, trait_basis)


def plain(panel, pheno, kin_values, trait_values, trait_basis):
    col_count = lax.axis_size("col")
    columns = pheno.shape[1]
    traits = trait_basis.shape[0]
    traits_here = traits // col_count
    set_count = columns // traits_here
    sets_dev = set_count // col_count
    whole_panel = lax.all_gather(panel, "col", axis=1, tiled=True)
    partial_value = lax.dot_general(
        whole_panel, pheno, (((0,), (0,)), ((), ())), preferred_element_type=jnp.float32
    )
    summed = lax.psum_scatter(partial_value, "row", scatter_dimension=0, tiled=True)
    first_row = lax.axis_index("row") * summed.shape[0]
    share_rows = summed.shape[0]
    by_trait = summed.reshape(share_rows, traits_here, set_count).transpose(0, 2, 1)
    by_trait = by_trait.reshape(share_rows, set_count * traits_here)
    grouped = lax.all_to_all(by_trait, "col", split_axis=1, concat_axis=1, tiled=True)
    grouped = grouped.reshape(share_rows, col_count, sets_dev, traits_here).transpose(0, 2, 1, 3)
    grouped = grouped.reshape(share_rows, sets_dev, traits)
    rotated = jnp.einsum("rst,tj->rsj", grouped, trait_basis, precision=HIGH)
    kin_rows = lax.dynamic_slice_in_dim(kin_values, first_row, share_rows, 0)
    product = kin_rows[:, None] * trait_values[None, :]
    scaled = rotated * (product / (product + 1.0))[:, None, :]
    unrotated = jnp.einsum("rsj,tj->rst", scaled, trait_basis, precision=HIGH)
    outgoing = unrotated.reshape(share_rows, sets_dev, col_count, traits_here).transpose(0, 2, 1, 3)
    outgoing = outgoing.reshape(share_rows, col_count * sets_dev * traits_here)
    returned = lax.all_to_all(outgoing, "col", split_axis=1, concat_axis=1, tiled=True)
    coeffs = returned.reshape(share_rows, set_count, traits_here).transpose(0, 2, 1)
    coeffs = coeffs.reshape(share_rows, columns)
    coeffs_low = lax.all_gather(coeffs.astype(jnp.bfloat16), "row", axis=0, tiled=True)
    genetic = jnp.dot(whole_panel, coeffs_low, preferred_element_type=jnp.float32)
    return (coeffs, genetic.astype(jnp.bfloat16))


def solution(mesh):
    return jax.shard_map(
        local,
        mesh=mesh,
        in_specs=(P("row", "col"), P("row", "col"), P(), P(), P()),
        out_specs=(P("row", "col"), P("row", "col")),
        check_vma=False,
    )
```

```python
import functools

import jax
import jax.numpy as jnp
from jax import lax
from jax.experimental import pallas as pl
from jax.experimental.pallas import tpu as pltpu
from jax.sharding import PartitionSpec as P

LANES = 128
PIECES = 8
EARLY = (0, 1, 2, 3, 4, 5)
LATE = (6, 7)
FROM_END = (1, 2, 3, 4, 5)
WAYS = (0, 1, 2, "y")
TILES = 16
MESH = pl.DeviceIdType.MESH
HIGH = lax.Precision.HIGHEST


def gather_rotate(
    rows, cols, q, pheno, basis_in, kin_in, trait_in,
    w_out, c_out,
    basis, kin, trait, g, ph, lent, acc, lent_acc, part_f, part, rparts, sb, rb, ob, crow, ct,
    load_sem, send_sem, recv_sem, lend_send, lend_recv,
    rs_send, rs_recv, a1_send, a1_recv, a2_send, a2_recv, ag_send, ag_recv,
):
    me_r, me_c = lax.axis_index("row"), lax.axis_index("col")
    lines = cols // 2
    z, y = me_c // 2, lax.rem(me_c, 2)
    width, people = q.shape
    piece = people // PIECES
    columns = pheno.shape[1]
    traits = basis.shape[0]
    sets = columns * cols // traits
    t_here = traits // cols
    late = people * len(LATE) // PIECES
    lot = late // PIECES

    own_load = pltpu.make_async_copy(q, g.at[me_c], load_sem.at[0])
    own_load.start()
    ph_load = pltpu.make_async_copy(pheno, ph, load_sem.at[1])
    ph_load.start()
    small = [
        pltpu.make_async_copy(a, b, load_sem.at[2 + i])
        for i, (a, b) in enumerate(((basis_in, basis), (kin_in, kin), (trait_in, trait)))
    ]
    for copy in small:
        copy.start()

    barrier = pltpu.get_barrier_semaphore()
    for d in range(1, cols):
        pl.semaphore_signal(barrier, inc=1, device_id=(me_r, lax.rem(me_c + d, cols)), device_id_type=MESH)
    for d in range(1, rows):
        pl.semaphore_signal(barrier, inc=1, device_id=(lax.rem(me_r + d, rows), me_c), device_id_type=MESH)
    pl.semaphore_wait(barrier, cols + rows - 2)

    far = z // (lines // 2)
    place_of = lambda k: k + far * (lines - 1 - 2 * k)
    is_end = z == place_of(0)
    is_mid = jnp.logical_not(is_end)
    own = lambda k: 2 * place_of(k) + y
    across = lambda k: 2 * place_of(k) + 1 - y
    SAME, OTHER = own, across

    def hop(way, kind, k, j):
        block = kind(k)
        target = me_c + 1 - 2 * y if way == "y" else own(way)
        here = g.at[block, :, pl.ds(j * piece, piece)]
        return pltpu.make_async_remote_copy(
            src_ref=here, dst_ref=here,
            send_sem=send_sem.at[WAYS.index(way), block, j], recv_sem=recv_sem.at[block, j],
            device_id=(me_r, target), device_id_type=MESH,
        )

    def lend(i):
        return pltpu.make_async_remote_copy(
            src_ref=pheno.at[pl.ds(people - late + i * lot, lot)], dst_ref=lent.at[pl.ds(i * lot, lot)],
            send_sem=lend_send.at[i], recv_sem=lend_recv.at[i],
            device_id=(me_r, own(1)), device_id_type=MESH,
        )

    def sender(role):
        def send(way, kind, k, j):
            role.append((way, kind, k, j))
            hop(way, kind, k, j).start()

        return send

    def arrived(kind, k, j):
        hop("y", kind, k, j).wait_recv()

    def lhs_of(k, j):
        pair = place_of(k)
        at = pl.ds(j * piece, piece)
        return pair, at, jnp.concatenate([g[2 * pair, :, at], g[2 * pair + 1, :, at]], axis=0)

    def turn(pair, at, lhs):
        w_out[at, pl.ds(pl.multiple_of(pair * LANES, LANES), LANES)] = lhs.T

    def process(k, j):
        pair, at, lhs = lhs_of(k, j)
        acc[pair] += jnp.dot(lhs, ph[at, :], preferred_element_type=jnp.float32)
        turn(pair, at, lhs)

    def process_lent(k, j):
        pair, _, lhs = lhs_of(k, j)
        theirs = lent[pl.ds((j - LATE[0]) * piece, piece), :]
        lent_acc[pair] += jnp.dot(lhs, theirs, preferred_element_type=jnp.float32)

    def reduce_copy(pair, h):
        return pltpu.make_async_remote_copy(
            src_ref=part.at[pair, h], dst_ref=rparts.at[me_r, h],
            send_sem=rs_send.at[pair, h], recv_sem=rs_recv.at[me_r, h],
            device_id=(pair, me_c), device_id_type=MESH,
        )

    def finish_pair(k, h=0):
        pair = place_of(k)

        @pl.when(pair != me_r)
        def _():
            part[pair, h] = (lent_acc if h else acc)[pair].astype(jnp.bfloat16)
            reduce_copy(pair, h).start()

    acc[...] = jnp.zeros_like(acc)
    own_load.wait()
    end_sent, mid_sent = [], []

    @pl.when(is_end)
    def _():
        send = sender(end_sent)
        for j in range(PIECES):
            send(1, SAME, 0, j)
            if j in EARLY:
                send("y", SAME, 0, j)
        for i in range(PIECES):
            lend(i).start()
        ph_load.wait()
        n = len(EARLY)
        h = n // 2
        for t in range(3 * n):
            line, j = t // n, t % n
            arrived(SAME, 1 + line, j)
            if line or j < h:
                send("y", SAME, 1 + line, j)
            if line == 0:
                arrived(OTHER, 0, j)
                if j in FROM_END:
                    send(1, OTHER, 0, j)
                process(0, j)
            elif t < n + h:
                arrived(OTHER, 1, j)
                process(1, j)
            elif t < 2 * n + h:
                arrived(OTHER, 2, t - n - h)
                process(2, t - n - h)
            else:
                arrived(OTHER, 3, t - 2 * n - h)
                process(3, t - 2 * n - h)
            if t == n - 1:
                finish_pair(0)
            if t == 2 * n + h - 1:
                finish_pair(2)
        for j in range(h, n):
            arrived(OTHER, 1, j)
            process(1, j)
            if j == n - 1:
                finish_pair(1)
            arrived(OTHER, 3, j)
            process(3, j)
        finish_pair(3)

    @pl.when(is_mid)
    def _():
        send = sender(mid_sent)
        n = len(EARLY)
        for j in range(PIECES):
            if j in EARLY:
                send(0, SAME, 1, j)
                send(2, SAME, 1, j)
            send("y", SAME, 1, j)
        lent_acc[...] = jnp.zeros_like(lent_acc)
        ph_load.wait()
        for j in range(PIECES):
            arrived(SAME, 0, j)
            if j in EARLY:
                send(2, SAME, 0, j)
            if j not in FROM_END:
                send("y", SAME, 0, j)
            if j in EARLY:
                arrived(SAME, 2, j)
                send(0, SAME, 2, j)
                if j not in FROM_END:
                    send("y", SAME, 2, j)
            if j == n - 1:
                for i in LATE:
                    send(2, SAME, 1, i)
            if j in LATE:
                send(2, SAME, 0, j)
                arrived(SAME, 3, j - n)
                send(0, SAME, 3, j - n)
                send("y", SAME, 3, j - n)
            arrived(OTHER, 1, j)
            process(1, j)
        for j in FROM_END:
            send(2, OTHER, 1, j)
        finish_pair(1)
        first = [j for j in range(PIECES) if j not in FROM_END]
        b = len(LATE)
        order = [(0, first[0]), (2, first[0])] + [(0, j) for j in first[1:]]
        for i, (k, j) in enumerate(order):
            lend(i).wait_recv()
            arrived(SAME, 3, b + i)
            send(0, SAME, 3, b + i)
            send("y", SAME, 3, b + i)
            arrived(OTHER, k, j)
            process(k, j)
        for j in EARLY[n // 2:]:
            send(0, OTHER, 1, j)
        for k in (0, 1):
            process_lent(k, LATE[0])
        done = len(order)
        for i, (k, j) in enumerate([(2, j) for j in LATE] + [(3, j) for j in LATE]):
            lend(done + i).wait_recv()
            arrived(SAME, k, j)
            send("y", SAME, k, j)
            arrived(OTHER, 3, i)
            process(3, i)
        for k in (0, 1):
            process_lent(k, LATE[1])
            finish_pair(k, 1)
        rest = [(3, j) for j in EARLY[2 * b:]] + [(2, j) for j in LATE] + [(3, j) for j in LATE]
        for i, j in enumerate(FROM_END):
            arrived(OTHER, 0, j)
            process(0, j)
            arrived(OTHER, 2, j)
            process(2, j)
            k, m = rest.pop(0)
            arrived(OTHER, k, m)
            process(k, m)
            if m in LATE:
                process_lent(k, m)
        finish_pair(0)
        finish_pair(2)
        finish_pair(2, 1)
        for k, m in rest:
            arrived(OTHER, k, m)
            process(k, m)
            process_lent(k, m)
        finish_pair(3)
        finish_pair(3, 1)

    end_bulk = [(None, SAME, 0, j) for j in LATE]
    end_bulk += [("z", SAME, 1, LATE[0])]
    end_bulk += [("z", SAME, k, j) for k in (2, 3) for j in LATE]
    mid_bulk = [(SAME, k, j) for k in (1, 2, 3) for j in LATE] + [(OTHER, 1, LATE[1])]

    def bulk(end_from, end_to, mid_from, mid_to):
        @pl.when(is_end)
        def _():
            send = sender(end_sent)
            for wait, kind, k, j in end_bulk[end_from:end_to]:
                if wait:
                    arrived(kind, k, j)
                send("y", kind, k, j)

        @pl.when(is_mid)
        def _():
            send = sender(mid_sent)
            for kind, k, j in mid_bulk[mid_from:mid_to]:
                send(0, kind, k, j)

    bulk(0, 2, 0, 2)

    def total_of(h):
        total = (lent_acc if h else acc)[me_r]
        for d in range(1, rows):
            src = lax.rem(me_r + d, rows)
            pltpu.make_async_remote_copy(
                src_ref=part.at[src, h], dst_ref=rparts.at[src, h],
                send_sem=rs_send.at[src, h], recv_sem=rs_recv.at[src, h],
                device_id=(src, me_c), device_id_type=MESH,
            ).wait_recv()
            total = total + rparts[src, h].astype(jnp.float32)
        part_f[...] = total.T
        by_set = [part_f[pl.ds(s, t_here, stride=sets), :] for s in range(sets)]
        turned = jnp.concatenate(by_set, axis=0).astype(jnp.bfloat16)
        sb[:, h] = turned.reshape(cols, columns // cols, LANES)

    total_of(0)

    @pl.when(is_mid)
    def _():
        total_of(1)

    @pl.when(is_end)
    def _():
        sb[:, 1] = jnp.zeros_like(sb[:, 1])

    def trade1(peer, slot):
        return pltpu.make_async_remote_copy(
            src_ref=sb.at[peer], dst_ref=rb.at[slot], send_sem=a1_send.at[peer], recv_sem=a1_recv.at[slot],
            device_id=(me_r, peer), device_id_type=MESH,
        )

    def trade2(peer, slot):
        return pltpu.make_async_remote_copy(
            src_ref=ob.at[peer], dst_ref=crow.at[me_r, slot], send_sem=a2_send.at[peer], recv_sem=a2_recv.at[slot],
            device_id=(me_r, peer), device_id_type=MESH,
        )

    def share(peer, slot):
        return pltpu.make_async_remote_copy(
            src_ref=crow.at[me_r], dst_ref=crow.at[slot], send_sem=ag_send.at[peer], recv_sem=ag_recv.at[slot],
            device_id=(peer, me_c), device_id_type=MESH,
        )

    col_peers = [lax.rem(me_c + d, cols) for d in range(1, cols)]
    row_peers = [lax.rem(me_r + d, rows) for d in range(1, rows)]
    for p in col_peers:
        trade1(p, me_c).start()
    bulk(2, 3, 2, 4)
    rb[me_c] = sb[me_c]
    for copy in small:
        copy.wait()
    product = kin[pl.ds(me_r, 1), :] * jnp.broadcast_to(trait[...], (LANES, traits)).T
    weight = product / (product + 1.0)
    for p in col_peers:
        trade1(p, p).wait_recv()
    s_here = sets // cols

    def gathered(s):
        at = slice(s * t_here, (s + 1) * t_here)
        terms = []
        for c in range(cols):
            term = rb[c, 0, at, :].astype(jnp.float32)
            if c // 2 in (0, lines - 1):
                term = term + rb[c + 2 if c // 2 == 0 else c - 2, 1, at, :].astype(jnp.float32)
            terms.append(term)
        return jnp.concatenate(terms, axis=0)

    got = jnp.concatenate([gathered(s) for s in range(s_here)], axis=1)
    rotated = jnp.dot(basis[...].T, got, precision=HIGH, preferred_element_type=jnp.float32)
    scaled = rotated * jnp.concatenate([weight] * s_here, axis=1)
    back = jnp.dot(basis[...], scaled, precision=HIGH, preferred_element_type=jnp.float32)
    for s in range(s_here):
        ob[:, s * t_here:(s + 1) * t_here, :] = (
            back[:, s * LANES:(s + 1) * LANES].reshape(cols, t_here, LANES).astype(jnp.bfloat16)
        )
    for p in col_peers:
        trade2(p, me_c).start()
    bulk(3, 5, 4, 6)
    crow[me_r, me_c] = ob[me_c]
    for p in col_peers:
        trade2(p, p).wait_recv()
    for p in row_peers:
        share(p, me_r).start()
    bulk(5, 7, 6, 7)

    def place(r):
        for s in range(sets):
            part_s = crow[r, s // s_here, (s % s_here) * t_here:(s % s_here + 1) * t_here, :]
            ct[pl.ds(s, t_here, stride=sets), :] = part_s.astype(jnp.float32)
        c_out[pl.ds(pl.multiple_of(r * LANES, LANES), LANES), :] = ct[...].T.astype(jnp.bfloat16)

    place(me_r)
    for p in row_peers:
        share(p, p).wait_recv()
        place(p)

    def turn_late(k, j):
        turn(*lhs_of(k, j))

    @pl.when(is_end)
    def _():
        waited = [(kind, k, j) for wait, kind, k, j in end_bulk if wait]
        for k in range(lines):
            for j in LATE:
                for kind in (SAME, OTHER):
                    if (kind, k) != (SAME, 0) and (kind, k, j) not in waited:
                        arrived(kind, k, j)
                turn_late(k, j)
        for way, kind, k, j in end_sent:
            hop(way, kind, k, j).wait_send()
        for i in range(PIECES):
            lend(i).wait_send()

    @pl.when(is_mid)
    def _():
        for way, kind, k, j in mid_sent:
            hop(way, kind, k, j).wait_send()
        for p in row_peers:
            reduce_copy(p, 1).wait_send()

    for p in row_peers:
        reduce_copy(p, 0).wait_send()
        share(p, me_r).wait_send()
    for p in col_peers:
        trade1(p, me_c).wait_send()
        trade2(p, me_c).wait_send()


def predict(w, c, gen_out, coeffs, held, gen_sem):
    share = coeffs.shape[0]
    size = w.shape[0] // TILES

    def emit(i):
        at = pl.ds(pl.multiple_of(i * size, size), size)
        return pltpu.make_async_copy(held.at[at], gen_out.at[at], gen_sem.at[i])

    def step(i, _):
        at = pl.ds(pl.multiple_of(i * size, size), size)
        held[at, :] = jnp.dot(w[at, :], c[...], preferred_element_type=jnp.float32).astype(jnp.bfloat16)
        emit(i).start()
        return 0

    lax.fori_loop(0, TILES, step, 0)
    mine = pl.ds(pl.multiple_of(lax.axis_index("row") * share, share), share)
    coeffs[...] = c[mine, :].astype(jnp.float32)

    def finish(i, _):
        emit(i).wait()
        return 0

    lax.fori_loop(0, TILES, finish, 0)


def fused(panel, pheno, kin_values, trait_values, trait_basis):
    rows, cols = lax.axis_size("row"), lax.axis_size("col")
    ind, columns = pheno.shape
    traits = trait_basis.shape[0]
    sets = columns * cols // traits
    share = kin_values.shape[0] // rows
    bf, f32 = jnp.bfloat16, jnp.float32
    hbm = pl.BlockSpec(memory_space=pltpu.HBM)
    vmem = pl.BlockSpec(memory_space=pltpu.VMEM)
    lot = columns // cols
    dma = pltpu.SemaphoreType.DMA
    given = (panel.T, pheno, trait_basis, kin_values.reshape(rows, share), trait_values[None, :])
    whole, low = pl.pallas_call(
        functools.partial(gather_rotate, rows, cols),
        out_shape=(
            pltpu.VMEM((ind, rows * share), bf),
            pltpu.VMEM((rows * share, columns), bf),
        ),
        in_specs=[hbm] * 5,
        out_specs=(vmem, vmem),
        scratch_shapes=[
            pltpu.VMEM((traits, traits), f32),
            pltpu.VMEM((rows, share), f32),
            pltpu.VMEM((1, traits), f32),
            pltpu.VMEM((cols, panel.shape[1], ind), bf),
            pltpu.VMEM((ind, columns), bf),
            pltpu.VMEM((ind * len(LATE) // PIECES, columns), bf),
            pltpu.VMEM((rows, share, columns), f32),
            pltpu.VMEM((rows, share, columns), f32),
            pltpu.VMEM((columns, LANES), f32),
            pltpu.VMEM((rows, 2, share, columns), bf),
            pltpu.VMEM((rows, 2, share, columns), bf),
            pltpu.VMEM((cols, 2, lot, LANES), bf),
            pltpu.VMEM((cols, 2, lot, LANES), bf),
            pltpu.VMEM((cols, lot, LANES), bf),
            pltpu.VMEM((rows, cols, lot, LANES), bf),
            pltpu.VMEM((columns, LANES), f32),
            dma((5,)), dma((len(WAYS), cols, PIECES)), dma((cols, PIECES)), dma((PIECES,)), dma((PIECES,)),
            dma((rows, 2)), dma((rows, 2)), dma((cols,)), dma((cols,)), dma((cols,)), dma((cols,)),
            dma((rows,)), dma((rows,)),
        ],
        compiler_params=pltpu.CompilerParams(
            collective_id=0, has_side_effects=True, vmem_limit_bytes=36 * 1024 * 1024
        ),
    )(*(pltpu.with_memory_space_constraint(a, pltpu.HBM) for a in given))
    genetic, coeffs = pl.pallas_call(
        predict,
        out_shape=(
            jax.ShapeDtypeStruct((ind, columns), bf),
            jax.ShapeDtypeStruct((share, columns), f32),
        ),
        in_specs=[vmem] * 2,
        out_specs=(hbm, vmem),
        scratch_shapes=[pltpu.VMEM((ind, columns), bf), dma((TILES,))],
        compiler_params=pltpu.CompilerParams(vmem_limit_bytes=20 * 1024 * 1024),
    )(whole, low)
    return coeffs, genetic


def local(panel, pheno, kin_values, trait_values, trait_basis):
    rows, cols = lax.axis_size("row"), lax.axis_size("col")
    eigen = kin_values.shape[0]
    fits = 2 * panel.shape[1] == LANES and eigen // rows == LANES and trait_basis.shape[0] // cols == 16
    if fits and rows == 4 and cols == 2 * rows:
        return fused(panel, pheno, kin_values, trait_values, trait_basis)
    return plain(panel, pheno, kin_values, trait_values, trait_basis)


def plain(panel, pheno, kin_values, trait_values, trait_basis):
    col_count = lax.axis_size("col")
    columns = pheno.shape[1]
    traits = trait_basis.shape[0]
    traits_here = traits // col_count
    set_count = columns // traits_here
    sets_dev = set_count // col_count
    whole_panel = lax.all_gather(panel, "col", axis=1, tiled=True)
    partial_value = lax.dot_general(
        whole_panel, pheno, (((0,), (0,)), ((), ())), preferred_element_type=jnp.float32
    )
    summed = lax.psum_scatter(partial_value, "row", scatter_dimension=0, tiled=True)
    first_row = lax.axis_index("row") * summed.shape[0]
    share_rows = summed.shape[0]
    by_trait = summed.reshape(share_rows, traits_here, set_count).transpose(0, 2, 1)
    by_trait = by_trait.reshape(share_rows, set_count * traits_here)
    grouped = lax.all_to_all(by_trait, "col", split_axis=1, concat_axis=1, tiled=True)
    grouped = grouped.reshape(share_rows, col_count, sets_dev, traits_here).transpose(0, 2, 1, 3)
    grouped = grouped.reshape(share_rows, sets_dev, traits)
    rotated = jnp.einsum("rst,tj->rsj", grouped, trait_basis, precision=HIGH)
    kin_rows = lax.dynamic_slice_in_dim(kin_values, first_row, share_rows, 0)
    product = kin_rows[:, None] * trait_values[None, :]
    scaled = rotated * (product / (product + 1.0))[:, None, :]
    unrotated = jnp.einsum("rsj,tj->rst", scaled, trait_basis, precision=HIGH)
    outgoing = unrotated.reshape(share_rows, sets_dev, col_count, traits_here).transpose(0, 2, 1, 3)
    outgoing = outgoing.reshape(share_rows, col_count * sets_dev * traits_here)
    returned = lax.all_to_all(outgoing, "col", split_axis=1, concat_axis=1, tiled=True)
    coeffs = returned.reshape(share_rows, set_count, traits_here).transpose(0, 2, 1)
    coeffs = coeffs.reshape(share_rows, columns)
    coeffs_low = lax.all_gather(coeffs.astype(jnp.bfloat16), "row", axis=0, tiled=True)
    genetic = jnp.dot(whole_panel, coeffs_low, preferred_element_type=jnp.float32)
    return (coeffs, genetic.astype(jnp.bfloat16))


def solution(mesh):
    return jax.shard_map(
        local,
        mesh=mesh,
        in_specs=(P("row", "col"), P("row", "col"), P(), P(), P()),
        out_specs=(P("row", "col"), P("row", "col")),
        check_vma=False,
    )
```

```python
import functools

import jax
import jax.numpy as jnp
from jax import lax
from jax.experimental import pallas as pl
from jax.experimental.pallas import tpu as pltpu
from jax.sharding import PartitionSpec as P

LANES = 128
PIECES = 8
EARLY = (0, 1, 2, 3, 4, 5)
LATE = (6, 7)
FROM_END = (1, 2, 3, 4, 5)
MID_FEED = 2
UNITS = 4
END_STEPS = (
    ("P10", "P11"),
    ("P20", "T00", "P21", "T01"),
    ("P22", "T02"),
    ("T03", "P23", "P30", "T10", "T11", "P31", "T20"),
    ("P32", "P33", "T21", "T22", "T23"),
    ("T30", "T31", "T32", "T33", "B12", "B13"),
)
MID_STEPS = (
    ("O10", "O11", "O20", "O21", "O22"),
    ("O23", "O30"),
    ("O31", "O32"),
    ("O33", "O12", "O13"),
    ("X12", "X13"),
    (),
)
TILES = 16
MESH = pl.DeviceIdType.MESH
HIGH = lax.Precision.HIGHEST


def gather_rotate(
    rows, cols, q, pheno, basis_in, kin_in, trait_in,
    w_out, c_out,
    basis, kin, trait, g, ph, lent, acc, lent_acc, part_f, part, rparts, sb, rb, ob, crow, ct,
    load_sem, bulk_send, recv_sem, lend_recv, small_send, rs_recv, trade_recv, ag_recv,
):
    me_r, me_c = lax.axis_index("row"), lax.axis_index("col")
    lines = cols // 2
    z, y = me_c // 2, lax.rem(me_c, 2)
    width, people = q.shape
    piece = people // PIECES
    columns = pheno.shape[1]
    traits = basis.shape[0]
    sets = columns * cols // traits
    t_here = traits // cols
    late = people * len(LATE) // PIECES
    lot = late // PIECES

    own_load = pltpu.make_async_copy(q, g.at[me_c], load_sem.at[0])
    own_load.start()
    ph_load = pltpu.make_async_copy(pheno, ph, load_sem.at[1])
    ph_load.start()
    small = [
        pltpu.make_async_copy(a, b, load_sem.at[2 + i])
        for i, (a, b) in enumerate(((basis_in, basis), (kin_in, kin), (trait_in, trait)))
    ]
    for copy in small:
        copy.start()

    barrier = pltpu.get_barrier_semaphore()
    for d in range(1, cols):
        pl.semaphore_signal(barrier, inc=1, device_id=(me_r, lax.rem(me_c + d, cols)), device_id_type=MESH)
    for d in range(1, rows):
        pl.semaphore_signal(barrier, inc=1, device_id=(lax.rem(me_r + d, rows), me_c), device_id_type=MESH)
    pl.semaphore_wait(barrier, cols + rows - 2)

    far = z // (lines // 2)
    place_of = lambda k: k + far * (lines - 1 - 2 * k)
    is_end = z == place_of(0)
    is_mid = jnp.logical_not(is_end)
    own = lambda k: 2 * place_of(k) + y
    across = lambda k: 2 * place_of(k) + 1 - y
    SAME, OTHER = own, across


    def bank(way):
        return 0 if way in (0, 1) else 1

    def sends_done(counts):
        for i, count in enumerate(counts):
            rows_of = w_out.at[pl.ds(0, count * width * piece // w_out.shape[1])]
            pltpu.make_async_copy(rows_of, rows_of, bulk_send.at[i]).wait()

    def hop(way, kind, k, j):
        block = kind(k)
        target = me_c + 1 - 2 * y if way == "y" else own(way)
        here = g.at[block, :, pl.ds(j * piece, piece)]
        return pltpu.make_async_remote_copy(
            src_ref=here, dst_ref=here,
            send_sem=bulk_send.at[bank(way)], recv_sem=recv_sem.at[block, j],
            device_id=(me_r, target), device_id_type=MESH,
        )

    def lend(i):
        return pltpu.make_async_remote_copy(
            src_ref=pheno.at[pl.ds(people - late + i * lot, lot)], dst_ref=lent.at[pl.ds(i * lot, lot)],
            send_sem=bulk_send.at[0], recv_sem=lend_recv.at[i * len(LATE) // PIECES],
            device_id=(me_r, own(1)), device_id_type=MESH,
        )

    def lent_here(i):
        there = lent.at[pl.ds(i * piece, piece)]
        pltpu.make_async_copy(there, there, lend_recv.at[i]).wait()

    def sender(role):
        def send(way, kind, k, j):
            role.append((way, kind, k, j))
            hop(way, kind, k, j).start()

        return send

    def arrived(kind, k, j):
        hop("y", kind, k, j).wait_recv()

    def lhs_of(k, at):
        pair = place_of(k)
        return pair, at, jnp.concatenate([g[2 * pair, :, at], g[2 * pair + 1, :, at]], axis=0)

    def turn(pair, at, lhs):
        w_out[at, pl.ds(pl.multiple_of(pair * LANES, LANES), LANES)] = lhs.T

    def process(k, j):
        pair, at, lhs = lhs_of(k, pl.ds(j * piece, piece))
        acc[pair] += jnp.dot(lhs, ph[at, :], preferred_element_type=jnp.float32)
        turn(pair, at, lhs)

    def process_lent(k, j):
        pair, _, lhs = lhs_of(k, pl.ds(j * piece, piece))
        theirs = lent[pl.ds((j - LATE[0]) * piece, piece), :]
        lent_acc[pair] += jnp.dot(lhs, theirs, preferred_element_type=jnp.float32)

    def reduce_copy(pair, h):
        return pltpu.make_async_remote_copy(
            src_ref=part.at[h, pair], dst_ref=rparts.at[h, me_r],
            send_sem=small_send.at[h], recv_sem=rs_recv.at[h],
            device_id=(pair, me_c), device_id_type=MESH,
        )

    def finish_pair(k, h=0):
        pair = place_of(k)

        @pl.when(pair != me_r)
        def _():
            part[h, pair] = (lent_acc if h else acc)[pair].astype(jnp.bfloat16)
            reduce_copy(pair, h).start()

    def unit(u):
        size = late // UNITS
        return pl.ds(people - late + u * size, size)

    def late_hop(way, kind, k, u):
        block = kind(k)
        here = g.at[block, :, unit(u)]
        return pltpu.make_async_remote_copy(
            src_ref=here, dst_ref=here, send_sem=bulk_send.at[0], recv_sem=recv_sem.at[block, len(EARLY) + u],
            device_id=(me_r, me_c + 1 - 2 * y if way == "y" else own(way)), device_id_type=MESH,
        )

    late_sent = {"end": [], "mid": []}

    def late_send_off(role, way, kind, k, u):
        late_sent[role].append((way, kind, k, u))
        late_hop(way, kind, k, u).start()

    def late_steps(role, i):
        for what, k, u in (END_STEPS if role == "end" else MID_STEPS)[i]:
            k, u = int(k), int(u)
            if what == "P":
                late_hop("y", SAME, k, u).wait_recv()
                late_send_off(role, "y", SAME, k, u)
            elif what in "OX":
                late_send_off(role, 0, SAME if what == "O" else OTHER, k, u)
            else:
                if what == "B":
                    late_hop("y", SAME, k, u).wait_recv()
                late_hop("y", OTHER, k, u).wait_recv()
                turn(*lhs_of(k, unit(u)))

    acc[...] = jnp.zeros_like(acc)
    own_load.wait()
    end_sent, mid_sent = [], []

    @pl.when(is_end)
    def _():
        send = sender(end_sent)
        for j in range(PIECES):
            send(1, SAME, 0, j)
            if j in EARLY:
                send("y", SAME, 0, j)
        for i in range(PIECES):
            lend(i).start()
        ph_load.wait()
        n = len(EARLY)
        h = n // 2
        for t in range(3 * n):
            line, j = t // n, t % n
            arrived(SAME, 1 + line, j)
            if line or j < h:
                send("y", SAME, 1 + line, j)
            if line == 0:
                arrived(OTHER, 0, j)
                if j in FROM_END:
                    send(1, OTHER, 0, j)
                process(0, j)
            elif t < n + h:
                arrived(OTHER, 1, j)
                process(1, j)
            elif t < 2 * n + h:
                arrived(OTHER, 2, t - n - h)
                process(2, t - n - h)
            else:
                arrived(OTHER, 3, t - 2 * n - h)
                process(3, t - 2 * n - h)
            if t == n - 1:
                finish_pair(0)
            if t == 2 * n + h - 1:
                finish_pair(2)
        for u in range(UNITS):
            late_send_off("end", "y", SAME, 0, u)
        for j in range(h, n):
            arrived(OTHER, 1, j)
            process(1, j)
            if j == n - 1:
                finish_pair(1)
            arrived(OTHER, 3, j)
            process(3, j)
        finish_pair(3)
        late_steps("end", 0)

    @pl.when(is_mid)
    def _():
        send = sender(mid_sent)
        n = len(EARLY)
        for j in range(PIECES):
            if j in EARLY:
                send(0, SAME, 1, j)
                send(2, SAME, 1, j)
            send("y", SAME, 1, j)
        lent_acc[...] = jnp.zeros_like(lent_acc)
        ph_load.wait()
        for j in range(PIECES):
            arrived(SAME, 0, j)
            if j in EARLY:
                send(2, SAME, 0, j)
            if j not in FROM_END:
                send("y", SAME, 0, j)
            if j in EARLY:
                arrived(SAME, 2, j)
                send(0, SAME, 2, j)
                if j not in FROM_END:
                    send("y", SAME, 2, j)
            if j == n - 1:
                for i in LATE:
                    send(2, SAME, 1, i)
            if j in LATE:
                send(2, SAME, 0, j)
                arrived(SAME, 3, j - n)
                send(0, SAME, 3, j - n)
                send("y", SAME, 3, j - n)
            arrived(OTHER, 1, j)
            process(1, j)
        for j in FROM_END:
            send(2, OTHER, 1, j)
        finish_pair(1)
        first = [j for j in range(PIECES) if j not in FROM_END]
        b = len(LATE)
        order = [(0, first[0]), (2, first[0])] + [(0, j) for j in first[1:]]
        for i, (k, j) in enumerate(order):
            arrived(SAME, 3, b + i)
            send(0, SAME, 3, b + i)
            send("y", SAME, 3, b + i)
            arrived(OTHER, k, j)
            process(k, j)
        for j in EARLY[n // 2:]:
            send(0, OTHER, 1, j)
        lent_here(0)
        for k in (0, 1):
            process_lent(k, LATE[0])
        for i, (k, j) in enumerate([(2, j) for j in LATE] + [(3, j) for j in LATE]):
            arrived(SAME, k, j)
            send("y", SAME, k, j)
            arrived(OTHER, 3, i)
            process(3, i)
        lent_here(1)
        for k in (0, 1):
            process_lent(k, LATE[1])
            finish_pair(k, 1)
        rest = [(3, j) for j in EARLY[2 * b:]] + [(2, j) for j in LATE] + [(3, j) for j in LATE]
        for i, j in enumerate(FROM_END):
            arrived(OTHER, 0, j)
            process(0, j)
            arrived(OTHER, 2, j)
            process(2, j)
            k, m = rest.pop(0)
            arrived(OTHER, k, m)
            process(k, m)
            if m in LATE:
                process_lent(k, m)
            if i == MID_FEED:
                late_steps("mid", 0)
        finish_pair(0)
        finish_pair(2)
        finish_pair(2, 1)
        for k, m in rest:
            arrived(OTHER, k, m)
            process(k, m)
            process_lent(k, m)
        finish_pair(3)
        finish_pair(3, 1)

    def exchange_time(i):
        @pl.when(is_end)
        def _():
            late_steps("end", i)

        @pl.when(is_mid)
        def _():
            late_steps("mid", i)

    def all_but_one(ref, sem):
        some = ref.at[pl.ds(0, ref.shape[0] - 1)]
        pltpu.make_async_copy(some, some, sem).wait()

    def total_of(h):
        all_but_one(rparts.at[h], rs_recv.at[h])
        total = (lent_acc if h else acc)[me_r]
        for d in range(1, rows):
            total = total + rparts[h, lax.rem(me_r + d, rows)].astype(jnp.float32)
        part_f[...] = total.T
        by_set = [part_f[pl.ds(s, t_here, stride=sets), :] for s in range(sets)]
        turned = jnp.concatenate(by_set, axis=0).astype(jnp.bfloat16)
        sb[:, h] = turned.reshape(cols, columns // cols, LANES)

    total_of(0)

    @pl.when(is_mid)
    def _():
        total_of(1)

    @pl.when(is_end)
    def _():
        sb[:, 1] = jnp.zeros_like(sb[:, 1])

    def trade1(peer, slot):
        return pltpu.make_async_remote_copy(
            src_ref=sb.at[peer], dst_ref=rb.at[slot], send_sem=small_send.at[2], recv_sem=trade_recv.at[0],
            device_id=(me_r, peer), device_id_type=MESH,
        )

    def trade2(peer, slot):
        return pltpu.make_async_remote_copy(
            src_ref=ob.at[peer], dst_ref=crow.at[me_r, slot], send_sem=small_send.at[3], recv_sem=trade_recv.at[1],
            device_id=(me_r, peer), device_id_type=MESH,
        )

    def share(peer, slot):
        return pltpu.make_async_remote_copy(
            src_ref=crow.at[me_r], dst_ref=crow.at[slot], send_sem=small_send.at[4], recv_sem=ag_recv.at[slot],
            device_id=(peer, me_c), device_id_type=MESH,
        )

    col_peers = [lax.rem(me_c + d, cols) for d in range(1, cols)]
    row_peers = [lax.rem(me_r + d, rows) for d in range(1, rows)]
    for p in col_peers:
        trade1(p, me_c).start()
    exchange_time(1)
    exchange_time(2)
    rb[me_c] = sb[me_c]
    for copy in small:
        copy.wait()
    product = kin[pl.ds(me_r, 1), :] * jnp.broadcast_to(trait[...], (LANES, traits)).T
    weight = product / (product + 1.0)
    all_but_one(rb, trade_recv.at[0])
    s_here = sets // cols

    def gathered(s):
        at = slice(s * t_here, (s + 1) * t_here)
        terms = []
        for c in range(cols):
            term = rb[c, 0, at, :].astype(jnp.float32)
            if c // 2 in (0, lines - 1):
                term = term + rb[c + 2 if c // 2 == 0 else c - 2, 1, at, :].astype(jnp.float32)
            terms.append(term)
        return jnp.concatenate(terms, axis=0)

    got = jnp.concatenate([gathered(s) for s in range(s_here)], axis=1)
    rotated = jnp.dot(basis[...].T, got, precision=HIGH, preferred_element_type=jnp.float32)
    scaled = rotated * jnp.concatenate([weight] * s_here, axis=1)
    back = jnp.dot(basis[...], scaled, precision=HIGH, preferred_element_type=jnp.float32)
    for s in range(s_here):
        ob[:, s * t_here:(s + 1) * t_here, :] = (
            back[:, s * LANES:(s + 1) * LANES].reshape(cols, t_here, LANES).astype(jnp.bfloat16)
        )
    for p in col_peers:
        trade2(p, me_c).start()
    exchange_time(3)
    crow[me_r, me_c] = ob[me_c]
    all_but_one(ob, trade_recv.at[1])
    for p in row_peers:
        share(p, me_r).start()

    def place(r):
        for s in range(sets):
            part_s = crow[r, s // s_here, (s % s_here) * t_here:(s % s_here + 1) * t_here, :]
            ct[pl.ds(s, t_here, stride=sets), :] = part_s.astype(jnp.float32)
        c_out[pl.ds(pl.multiple_of(r * LANES, LANES), LANES), :] = ct[...].T.astype(jnp.bfloat16)

    place(me_r)
    exchange_time(4)
    for p in row_peers:
        share(p, p).wait_recv()
        place(p)
    exchange_time(5)

    def count(sent, others, late):
        counts = [others + late * piece_of_unit, 0]
        for way, *_ in sent:
            counts[bank(way)] += 1
        return counts

    piece_of_unit = late / (UNITS * piece)

    @pl.when(is_end)
    def _():
        sends_done([int(c) for c in count(end_sent, PIECES, len(late_sent["end"]))])

    @pl.when(is_mid)
    def _():
        sends_done([int(c) for c in count(mid_sent, 0, len(late_sent["mid"]))])
        all_but_one(part.at[1], small_send.at[1])

    all_but_one(part.at[0], small_send.at[0])
    all_but_one(sb, small_send.at[2])
    all_but_one(ob, small_send.at[3])
    all_but_one(crow, small_send.at[4])


def predict(w, c, gen_out, coeffs_out, held, coeffs, gen_sem):
    share = coeffs.shape[0]
    size = w.shape[0] // TILES
    mine = pl.ds(pl.multiple_of(lax.axis_index("row") * share, share), share)
    coeffs[...] = c[mine, :].astype(jnp.float32)
    copies = [pltpu.make_async_copy(coeffs, coeffs_out, gen_sem.at[TILES])]
    copies[0].start()
    for i in range(TILES):
        at = pl.ds(i * size, size)
        held[at, :] = jnp.dot(w[at, :], c[...], preferred_element_type=jnp.float32).astype(jnp.bfloat16)
        copies.append(pltpu.make_async_copy(held.at[at], gen_out.at[at], gen_sem.at[i]))
        copies[-1].start()
    for copy in copies:
        copy.wait()


def fused(panel, pheno, kin_values, trait_values, trait_basis):
    rows, cols = lax.axis_size("row"), lax.axis_size("col")
    ind, columns = pheno.shape
    traits = trait_basis.shape[0]
    sets = columns * cols // traits
    share = kin_values.shape[0] // rows
    bf, f32 = jnp.bfloat16, jnp.float32
    hbm = pl.BlockSpec(memory_space=pltpu.HBM)
    vmem = pl.BlockSpec(memory_space=pltpu.VMEM)
    lot = columns // cols
    dma = pltpu.SemaphoreType.DMA
    given = (panel.T, pheno, trait_basis, kin_values.reshape(rows, share), trait_values[None, :])
    whole, low = pl.pallas_call(
        functools.partial(gather_rotate, rows, cols),
        out_shape=(
            pltpu.VMEM((ind, rows * share), bf),
            pltpu.VMEM((rows * share, columns), bf),
        ),
        in_specs=[hbm] * 5,
        out_specs=(vmem, vmem),
        scratch_shapes=[
            pltpu.VMEM((traits, traits), f32),
            pltpu.VMEM((rows, share), f32),
            pltpu.VMEM((1, traits), f32),
            pltpu.VMEM((cols, panel.shape[1], ind), bf),
            pltpu.VMEM((ind, columns), bf),
            pltpu.VMEM((ind * len(LATE) // PIECES, columns), bf),
            pltpu.VMEM((rows, share, columns), f32),
            pltpu.VMEM((rows, share, columns), f32),
            pltpu.VMEM((columns, LANES), f32),
            pltpu.VMEM((2, rows, share, columns), bf),
            pltpu.VMEM((2, rows, share, columns), bf),
            pltpu.VMEM((cols, 2, lot, LANES), bf),
            pltpu.VMEM((cols, 2, lot, LANES), bf),
            pltpu.VMEM((cols, lot, LANES), bf),
            pltpu.VMEM((rows, cols, lot, LANES), bf),
            pltpu.VMEM((columns, LANES), f32),
            dma((5,)), dma((2,)), dma((cols, len(EARLY) + UNITS)), dma((len(LATE),)), dma((5,)), dma((2,)), dma((2,)), dma((rows,)),
        ],
        compiler_params=pltpu.CompilerParams(
            collective_id=0, has_side_effects=True, vmem_limit_bytes=36 * 1024 * 1024
        ),
    )(*(pltpu.with_memory_space_constraint(a, pltpu.HBM) for a in given))
    genetic, coeffs = pl.pallas_call(
        predict,
        out_shape=(
            jax.ShapeDtypeStruct((ind, columns), bf),
            jax.ShapeDtypeStruct((share, columns), f32),
        ),
        in_specs=[vmem] * 2,
        out_specs=(hbm, hbm),
        scratch_shapes=[pltpu.VMEM((ind, columns), bf), pltpu.VMEM((share, columns), f32), dma((TILES + 1,))],
        compiler_params=pltpu.CompilerParams(vmem_limit_bytes=20 * 1024 * 1024),
    )(whole, low)
    return coeffs, genetic


def local(panel, pheno, kin_values, trait_values, trait_basis):
    rows, cols = lax.axis_size("row"), lax.axis_size("col")
    eigen = kin_values.shape[0]
    fits = 2 * panel.shape[1] == LANES and eigen // rows == LANES and trait_basis.shape[0] // cols == 16
    if fits and rows == 4 and cols == 2 * rows:
        return fused(panel, pheno, kin_values, trait_values, trait_basis)
    return plain(panel, pheno, kin_values, trait_values, trait_basis)


def plain(panel, pheno, kin_values, trait_values, trait_basis):
    col_count = lax.axis_size("col")
    columns = pheno.shape[1]
    traits = trait_basis.shape[0]
    traits_here = traits // col_count
    set_count = columns // traits_here
    sets_dev = set_count // col_count
    whole_panel = lax.all_gather(panel, "col", axis=1, tiled=True)
    partial_value = lax.dot_general(
        whole_panel, pheno, (((0,), (0,)), ((), ())), preferred_element_type=jnp.float32
    )
    summed = lax.psum_scatter(partial_value, "row", scatter_dimension=0, tiled=True)
    first_row = lax.axis_index("row") * summed.shape[0]
    share_rows = summed.shape[0]
    by_trait = summed.reshape(share_rows, traits_here, set_count).transpose(0, 2, 1)
    by_trait = by_trait.reshape(share_rows, set_count * traits_here)
    grouped = lax.all_to_all(by_trait, "col", split_axis=1, concat_axis=1, tiled=True)
    grouped = grouped.reshape(share_rows, col_count, sets_dev, traits_here).transpose(0, 2, 1, 3)
    grouped = grouped.reshape(share_rows, sets_dev, traits)
    rotated = jnp.einsum("rst,tj->rsj", grouped, trait_basis, precision=HIGH)
    kin_rows = lax.dynamic_slice_in_dim(kin_values, first_row, share_rows, 0)
    product = kin_rows[:, None] * trait_values[None, :]
    scaled = rotated * (product / (product + 1.0))[:, None, :]
    unrotated = jnp.einsum("rsj,tj->rst", scaled, trait_basis, precision=HIGH)
    outgoing = unrotated.reshape(share_rows, sets_dev, col_count, traits_here).transpose(0, 2, 1, 3)
    outgoing = outgoing.reshape(share_rows, col_count * sets_dev * traits_here)
    returned = lax.all_to_all(outgoing, "col", split_axis=1, concat_axis=1, tiled=True)
    coeffs = returned.reshape(share_rows, set_count, traits_here).transpose(0, 2, 1)
    coeffs = coeffs.reshape(share_rows, columns)
    coeffs_low = lax.all_gather(coeffs.astype(jnp.bfloat16), "row", axis=0, tiled=True)
    genetic = jnp.dot(whole_panel, coeffs_low, preferred_element_type=jnp.float32)
    return (coeffs, genetic.astype(jnp.bfloat16))


def solution(mesh):
    return jax.shard_map(
        local,
        mesh=mesh,
        in_specs=(P("row", "col"), P("row", "col"), P(), P(), P()),
        out_specs=(P("row", "col"), P("row", "col")),
        check_vma=False,
    )
```

```python
import functools

import jax
import jax.numpy as jnp
from jax import lax
from jax.experimental import pallas as pl
from jax.experimental.pallas import tpu as pltpu
from jax.sharding import PartitionSpec as P

LANES = 128
PIECES = 8
EARLY = (0, 1, 2, 3, 4, 5)
LATE = (6, 7)
FROM_END = (1, 2, 3, 4, 5)
MID_FEED = 2
UNITS = 4
END_STEPS = (
    ("P10", "P11"),
    ("P20", "T00", "P21", "T01"),
    ("P22", "T02"),
    ("T03", "P23", "P30", "T10", "T11", "P31", "T20"),
    ("P32", "P33", "T21", "T22", "T23"),
    ("T30", "T31", "T32", "T33", "B12", "B13"),
)
MID_STEPS = (
    ("O10", "O11", "O20", "O21", "O22"),
    ("O23", "O30"),
    ("O31", "O32"),
    ("O33", "O12", "O13"),
    ("X12", "X13"),
    (),
)
TILES = 16
MESH = pl.DeviceIdType.MESH
HIGH = lax.Precision.HIGHEST


def gather_rotate(
    rows, cols, q, pheno, basis_in, kin_in, trait_in,
    w_out, c_out,
    basis, kin, trait, g, ph, lent, acc, lent_acc, part_f, part, rparts, sb, rb, ob, crow, ct,
    load_sem, bulk_send, recv_sem, lend_recv, small_send, rs_recv, trade_recv, ag_recv,
):
    me_r, me_c = lax.axis_index("row"), lax.axis_index("col")
    lines = cols // 2
    z, y = me_c // 2, lax.rem(me_c, 2)
    width, people = q.shape
    piece = people // PIECES
    columns = pheno.shape[1]
    traits = basis.shape[0]
    sets = columns * cols // traits
    t_here = traits // cols
    late = people * len(LATE) // PIECES
    lot = late // PIECES

    own_load = pltpu.make_async_copy(q, g.at[me_c], load_sem.at[0])
    own_load.start()
    ph_load = pltpu.make_async_copy(pheno, ph, load_sem.at[1])
    ph_load.start()
    small = [
        pltpu.make_async_copy(a, b, load_sem.at[2 + i])
        for i, (a, b) in enumerate(((basis_in, basis), (kin_in, kin), (trait_in, trait)))
    ]
    for copy in small:
        copy.start()

    far = z // (lines // 2)
    place_of = lambda k: k + far * (lines - 1 - 2 * k)
    is_end = z == place_of(0)
    is_mid = jnp.logical_not(is_end)
    own = lambda k: 2 * place_of(k) + y

    barrier = pltpu.get_barrier_semaphore()

    def greet(r, c):
        pl.semaphore_signal(barrier, inc=1, device_id=(r, c), device_id_type=MESH)

    for d in range(1, rows):
        greet(lax.rem(me_r + d, rows), me_c)
    greet(me_r, me_c + 1 - 2 * y)

    @pl.when(is_end)
    def _():
        greet(me_r, own(1))
        pl.semaphore_wait(barrier, rows + 1)

    @pl.when(is_mid)
    def _():
        greet(me_r, own(0))
        greet(me_r, own(2))
        pl.semaphore_wait(barrier, rows + 2)

    across = lambda k: 2 * place_of(k) + 1 - y
    SAME, OTHER = own, across


    def bank(way):
        return 0 if way in (0, 1) else 1

    def sends_done(counts):
        for i, count in enumerate(counts):
            rows_of = w_out.at[pl.ds(0, count * width * piece // w_out.shape[1])]
            pltpu.make_async_copy(rows_of, rows_of, bulk_send.at[i]).wait()

    def hop(way, kind, k, j):
        block = kind(k)
        target = me_c + 1 - 2 * y if way == "y" else own(way)
        here = g.at[block, :, pl.ds(j * piece, piece)]
        return pltpu.make_async_remote_copy(
            src_ref=here, dst_ref=here,
            send_sem=bulk_send.at[bank(way)], recv_sem=recv_sem.at[block, j],
            device_id=(me_r, target), device_id_type=MESH,
        )

    def lend(i):
        return pltpu.make_async_remote_copy(
            src_ref=pheno.at[pl.ds(people - late + i * lot, lot)], dst_ref=lent.at[pl.ds(i * lot, lot)],
            send_sem=bulk_send.at[0], recv_sem=lend_recv.at[i * len(LATE) // PIECES],
            device_id=(me_r, own(1)), device_id_type=MESH,
        )

    def lent_here(i):
        there = lent.at[pl.ds(i * piece, piece)]
        pltpu.make_async_copy(there, there, lend_recv.at[i]).wait()

    def sender(role):
        def send(way, kind, k, j):
            role.append((way, kind, k, j))
            hop(way, kind, k, j).start()

        return send

    def arrived(kind, k, j):
        hop("y", kind, k, j).wait_recv()

    def lhs_of(k, at):
        pair = place_of(k)
        return pair, at, jnp.concatenate([g[2 * pair, :, at], g[2 * pair + 1, :, at]], axis=0)

    def turn(pair, at, lhs):
        w_out[at, pl.ds(pl.multiple_of(pair * LANES, LANES), LANES)] = lhs.T

    def process(k, j):
        pair, at, lhs = lhs_of(k, pl.ds(j * piece, piece))
        acc[pair] += jnp.dot(lhs, ph[at, :], preferred_element_type=jnp.float32)
        turn(pair, at, lhs)

    def process_lent(k, j):
        pair, _, lhs = lhs_of(k, pl.ds(j * piece, piece))
        theirs = lent[pl.ds((j - LATE[0]) * piece, piece), :]
        lent_acc[pair] += jnp.dot(lhs, theirs, preferred_element_type=jnp.float32)

    def reduce_copy(pair, h):
        return pltpu.make_async_remote_copy(
            src_ref=part.at[h, pair], dst_ref=rparts.at[h, me_r],
            send_sem=small_send.at[h], recv_sem=rs_recv.at[h],
            device_id=(pair, me_c), device_id_type=MESH,
        )

    def finish_pair(k, h=0):
        pair = place_of(k)

        @pl.when(pair != me_r)
        def _():
            part[h, pair] = (lent_acc if h else acc)[pair].astype(jnp.bfloat16)
            reduce_copy(pair, h).start()

    def unit(u):
        size = late // UNITS
        return pl.ds(people - late + u * size, size)

    def late_hop(way, kind, k, u):
        block = kind(k)
        here = g.at[block, :, unit(u)]
        return pltpu.make_async_remote_copy(
            src_ref=here, dst_ref=here, send_sem=bulk_send.at[0], recv_sem=recv_sem.at[block, len(EARLY) + u],
            device_id=(me_r, me_c + 1 - 2 * y if way == "y" else own(way)), device_id_type=MESH,
        )

    late_sent = {"end": [], "mid": []}

    def late_send_off(role, way, kind, k, u):
        late_sent[role].append((way, kind, k, u))
        late_hop(way, kind, k, u).start()

    def late_steps(role, i):
        for what, k, u in (END_STEPS if role == "end" else MID_STEPS)[i]:
            k, u = int(k), int(u)
            if what == "P":
                late_hop("y", SAME, k, u).wait_recv()
                late_send_off(role, "y", SAME, k, u)
            elif what in "OX":
                late_send_off(role, 0, SAME if what == "O" else OTHER, k, u)
            else:
                if what == "B":
                    late_hop("y", SAME, k, u).wait_recv()
                late_hop("y", OTHER, k, u).wait_recv()
                turn(*lhs_of(k, unit(u)))

    acc[...] = jnp.zeros_like(acc)
    own_load.wait()
    end_sent, mid_sent = [], []

    @pl.when(is_end)
    def _():
        send = sender(end_sent)
        for j in range(PIECES):
            send(1, SAME, 0, j)
            if j in EARLY:
                send("y", SAME, 0, j)
        for i in range(PIECES):
            lend(i).start()
        ph_load.wait()
        n = len(EARLY)
        h = n // 2
        for t in range(3 * n):
            line, j = t // n, t % n
            arrived(SAME, 1 + line, j)
            if line or j < h:
                send("y", SAME, 1 + line, j)
            if line == 0:
                arrived(OTHER, 0, j)
                if j in FROM_END:
                    send(1, OTHER, 0, j)
                process(0, j)
            elif t < n + h:
                arrived(OTHER, 1, j)
                process(1, j)
            elif t < 2 * n + h:
                arrived(OTHER, 2, t - n - h)
                process(2, t - n - h)
            else:
                arrived(OTHER, 3, t - 2 * n - h)
                process(3, t - 2 * n - h)
            if t == n - 1:
                finish_pair(0)
            if t == 2 * n + h - 1:
                finish_pair(2)
        for u in range(UNITS):
            late_send_off("end", "y", SAME, 0, u)
        for j in range(h, n):
            arrived(OTHER, 1, j)
            process(1, j)
            if j == n - 1:
                finish_pair(1)
            arrived(OTHER, 3, j)
            process(3, j)
        finish_pair(3)
        late_steps("end", 0)

    @pl.when(is_mid)
    def _():
        send = sender(mid_sent)
        n = len(EARLY)
        for j in range(PIECES):
            if j in EARLY:
                send(0, SAME, 1, j)
                send(2, SAME, 1, j)
            send("y", SAME, 1, j)
        lent_acc[...] = jnp.zeros_like(lent_acc)
        ph_load.wait()
        for j in range(PIECES):
            arrived(SAME, 0, j)
            if j in EARLY:
                send(2, SAME, 0, j)
            if j not in FROM_END:
                send("y", SAME, 0, j)
            if j in EARLY:
                arrived(SAME, 2, j)
                send(0, SAME, 2, j)
                if j not in FROM_END:
                    send("y", SAME, 2, j)
            if j == n - 1:
                for i in LATE:
                    send(2, SAME, 1, i)
            if j in LATE:
                send(2, SAME, 0, j)
                arrived(SAME, 3, j - n)
                send(0, SAME, 3, j - n)
                send("y", SAME, 3, j - n)
            arrived(OTHER, 1, j)
            process(1, j)
        for j in FROM_END:
            send(2, OTHER, 1, j)
        finish_pair(1)
        first = [j for j in range(PIECES) if j not in FROM_END]
        b = len(LATE)
        early_y = EARLY[: n // 2]
        for i, (k, j) in enumerate([(0, first[0]), (2, first[0]), (0, LATE[0]), (3, early_y[0])]):
            arrived(SAME, 3, b + i)
            send(0, SAME, 3, b + i)
            if b + i in early_y:
                send("y", SAME, 3, b + i)
            arrived(OTHER, k, j)
            process(k, j)
        for j in EARLY[n // 2:]:
            send(0, OTHER, 1, j)
        lent_here(0)
        for k in (0, 1):
            process_lent(k, LATE[0])
        here = [(2, j) for j in LATE] + [(3, j) for j in LATE]
        for (k, j), (m, i) in zip(here, [(0, LATE[1]), (3, early_y[1]), (3, early_y[2]), (2, LATE[0])]):
            arrived(SAME, k, j)
            send("y", SAME, k, j)
            arrived(OTHER, m, i)
            process(m, i)
        for j in EARLY[n // 2:]:
            send("y", SAME, 3, j)
        lent_here(1)
        for k in (0, 1):
            process_lent(k, LATE[1])
            finish_pair(k, 1)
        process_lent(2, LATE[0])
        rest = [(2, LATE[1]), (3, LATE[0]), (3, LATE[1])] + [(3, j) for j in EARLY[n // 2:]]
        for i, j in enumerate(FROM_END):
            arrived(OTHER, 0, j)
            process(0, j)
            arrived(OTHER, 2, j)
            process(2, j)
            k, m = rest.pop(0)
            arrived(OTHER, k, m)
            process(k, m)
            if m in LATE:
                process_lent(k, m)
            if m == LATE[1]:
                finish_pair(k, 1)
            if i == MID_FEED:
                late_steps("mid", 0)
        finish_pair(0)
        finish_pair(2)
        for k, m in rest:
            arrived(OTHER, k, m)
            process(k, m)
        finish_pair(3)

    def exchange_time(i):
        @pl.when(is_end)
        def _():
            late_steps("end", i)

        @pl.when(is_mid)
        def _():
            late_steps("mid", i)

    def all_but_one(ref, sem):
        some = ref.at[pl.ds(0, ref.shape[0] - 1)]
        pltpu.make_async_copy(some, some, sem).wait()

    def total_of(h):
        all_but_one(rparts.at[h], rs_recv.at[h])
        total = (lent_acc if h else acc)[me_r]
        for d in range(1, rows):
            total = total + rparts[h, lax.rem(me_r + d, rows)].astype(jnp.float32)
        part_f[...] = total.T
        by_set = [part_f[pl.ds(s, t_here, stride=sets), :] for s in range(sets)]
        turned = jnp.concatenate(by_set, axis=0).astype(jnp.bfloat16)
        sb[:, h] = turned.reshape(cols, columns // cols, LANES)

    total_of(0)

    @pl.when(is_mid)
    def _():
        total_of(1)

    @pl.when(is_end)
    def _():
        sb[:, 1] = jnp.zeros_like(sb[:, 1])

    def trade1(peer, slot):
        return pltpu.make_async_remote_copy(
            src_ref=sb.at[peer], dst_ref=rb.at[slot], send_sem=small_send.at[2], recv_sem=trade_recv.at[0],
            device_id=(me_r, peer), device_id_type=MESH,
        )

    def trade2(peer, slot):
        return pltpu.make_async_remote_copy(
            src_ref=ob.at[peer], dst_ref=crow.at[me_r, slot], send_sem=small_send.at[3], recv_sem=trade_recv.at[1],
            device_id=(me_r, peer), device_id_type=MESH,
        )

    def share(peer, slot):
        return pltpu.make_async_remote_copy(
            src_ref=crow.at[me_r], dst_ref=crow.at[slot], send_sem=small_send.at[4], recv_sem=ag_recv.at[slot],
            device_id=(peer, me_c), device_id_type=MESH,
        )

    col_peers = [lax.rem(me_c + d, cols) for d in range(1, cols)]
    row_peers = [lax.rem(me_r + d, rows) for d in range(1, rows)]
    for p in col_peers:
        trade1(p, me_c).start()
    exchange_time(1)
    exchange_time(2)
    rb[me_c] = sb[me_c]
    for copy in small:
        copy.wait()
    product = kin[pl.ds(me_r, 1), :] * jnp.broadcast_to(trait[...], (LANES, traits)).T
    weight = product / (product + 1.0)
    all_but_one(rb, trade_recv.at[0])
    s_here = sets // cols

    def gathered(s):
        at = slice(s * t_here, (s + 1) * t_here)
        terms = []
        for c in range(cols):
            term = rb[c, 0, at, :].astype(jnp.float32)
            if c // 2 in (0, lines - 1):
                term = term + rb[c + 2 if c // 2 == 0 else c - 2, 1, at, :].astype(jnp.float32)
            terms.append(term)
        return jnp.concatenate(terms, axis=0)

    got = jnp.concatenate([gathered(s) for s in range(s_here)], axis=1)
    rotated = jnp.dot(basis[...].T, got, precision=HIGH, preferred_element_type=jnp.float32)
    scaled = rotated * jnp.concatenate([weight] * s_here, axis=1)
    back = jnp.dot(basis[...], scaled, precision=HIGH, preferred_element_type=jnp.float32)
    for s in range(s_here):
        ob[:, s * t_here:(s + 1) * t_here, :] = (
            back[:, s * LANES:(s + 1) * LANES].reshape(cols, t_here, LANES).astype(jnp.bfloat16)
        )
    for p in col_peers:
        trade2(p, me_c).start()
    exchange_time(3)
    crow[me_r, me_c] = ob[me_c]
    all_but_one(ob, trade_recv.at[1])
    for p in row_peers:
        share(p, me_r).start()

    def place(r):
        for s in range(sets):
            part_s = crow[r, s // s_here, (s % s_here) * t_here:(s % s_here + 1) * t_here, :]
            ct[pl.ds(s, t_here, stride=sets), :] = part_s.astype(jnp.float32)
        c_out[pl.ds(pl.multiple_of(r * LANES, LANES), LANES), :] = ct[...].T.astype(jnp.bfloat16)

    place(me_r)
    exchange_time(4)
    for p in row_peers:
        share(p, p).wait_recv()
        place(p)
    exchange_time(5)

    def count(sent, others, late):
        counts = [others + late * piece_of_unit, 0]
        for way, *_ in sent:
            counts[bank(way)] += 1
        return counts

    piece_of_unit = late / (UNITS * piece)

    @pl.when(is_end)
    def _():
        sends_done([int(c) for c in count(end_sent, PIECES, len(late_sent["end"]))])

    @pl.when(is_mid)
    def _():
        sends_done([int(c) for c in count(mid_sent, 0, len(late_sent["mid"]))])
        all_but_one(part.at[1], small_send.at[1])

    all_but_one(part.at[0], small_send.at[0])
    all_but_one(sb, small_send.at[2])
    all_but_one(ob, small_send.at[3])
    all_but_one(crow, small_send.at[4])


def predict(w, c, gen_out, coeffs_out, held, coeffs, gen_sem):
    share = coeffs.shape[0]
    size = w.shape[0] // TILES
    mine = pl.ds(pl.multiple_of(lax.axis_index("row") * share, share), share)
    coeffs[...] = c[mine, :].astype(jnp.float32)
    copies = [pltpu.make_async_copy(coeffs, coeffs_out, gen_sem.at[TILES])]
    copies[0].start()
    for i in range(TILES):
        at = pl.ds(i * size, size)
        held[at, :] = jnp.dot(w[at, :], c[...], preferred_element_type=jnp.float32).astype(jnp.bfloat16)
        copies.append(pltpu.make_async_copy(held.at[at], gen_out.at[at], gen_sem.at[i]))
        copies[-1].start()
    for copy in copies:
        copy.wait()


def fused(panel, pheno, kin_values, trait_values, trait_basis):
    rows, cols = lax.axis_size("row"), lax.axis_size("col")
    ind, columns = pheno.shape
    traits = trait_basis.shape[0]
    sets = columns * cols // traits
    share = kin_values.shape[0] // rows
    bf, f32 = jnp.bfloat16, jnp.float32
    hbm = pl.BlockSpec(memory_space=pltpu.HBM)
    vmem = pl.BlockSpec(memory_space=pltpu.VMEM)
    lot = columns // cols
    dma = pltpu.SemaphoreType.DMA
    given = (panel.T, pheno, trait_basis, kin_values.reshape(rows, share), trait_values[None, :])
    whole, low = pl.pallas_call(
        functools.partial(gather_rotate, rows, cols),
        out_shape=(
            pltpu.VMEM((ind, rows * share), bf),
            pltpu.VMEM((rows * share, columns), bf),
        ),
        in_specs=[hbm] * 5,
        out_specs=(vmem, vmem),
        scratch_shapes=[
            pltpu.VMEM((traits, traits), f32),
            pltpu.VMEM((rows, share), f32),
            pltpu.VMEM((1, traits), f32),
            pltpu.VMEM((cols, panel.shape[1], ind), bf),
            pltpu.VMEM((ind, columns), bf),
            pltpu.VMEM((ind * len(LATE) // PIECES, columns), bf),
            pltpu.VMEM((rows, share, columns), f32),
            pltpu.VMEM((rows, share, columns), f32),
            pltpu.VMEM((columns, LANES), f32),
            pltpu.VMEM((2, rows, share, columns), bf),
            pltpu.VMEM((2, rows, share, columns), bf),
            pltpu.VMEM((cols, 2, lot, LANES), bf),
            pltpu.VMEM((cols, 2, lot, LANES), bf),
            pltpu.VMEM((cols, lot, LANES), bf),
            pltpu.VMEM((rows, cols, lot, LANES), bf),
            pltpu.VMEM((columns, LANES), f32),
            dma((5,)), dma((2,)), dma((cols, len(EARLY) + UNITS)), dma((len(LATE),)), dma((5,)), dma((2,)), dma((2,)), dma((rows,)),
        ],
        compiler_params=pltpu.CompilerParams(
            collective_id=0, has_side_effects=True, vmem_limit_bytes=36 * 1024 * 1024
        ),
    )(*(pltpu.with_memory_space_constraint(a, pltpu.HBM) for a in given))
    genetic, coeffs = pl.pallas_call(
        predict,
        out_shape=(
            jax.ShapeDtypeStruct((ind, columns), bf),
            jax.ShapeDtypeStruct((share, columns), f32),
        ),
        in_specs=[vmem] * 2,
        out_specs=(hbm, hbm),
        scratch_shapes=[pltpu.VMEM((ind, columns), bf), pltpu.VMEM((share, columns), f32), dma((TILES + 1,))],
        compiler_params=pltpu.CompilerParams(vmem_limit_bytes=20 * 1024 * 1024),
    )(whole, low)
    return coeffs, genetic


def local(panel, pheno, kin_values, trait_values, trait_basis):
    rows, cols = lax.axis_size("row"), lax.axis_size("col")
    eigen = kin_values.shape[0]
    fits = 2 * panel.shape[1] == LANES and eigen // rows == LANES and trait_basis.shape[0] // cols == 16
    if fits and rows == 4 and cols == 2 * rows:
        return fused(panel, pheno, kin_values, trait_values, trait_basis)
    return plain(panel, pheno, kin_values, trait_values, trait_basis)


def plain(panel, pheno, kin_values, trait_values, trait_basis):
    col_count = lax.axis_size("col")
    columns = pheno.shape[1]
    traits = trait_basis.shape[0]
    traits_here = traits // col_count
    set_count = columns // traits_here
    sets_dev = set_count // col_count
    whole_panel = lax.all_gather(panel, "col", axis=1, tiled=True)
    partial_value = lax.dot_general(
        whole_panel, pheno, (((0,), (0,)), ((), ())), preferred_element_type=jnp.float32
    )
    summed = lax.psum_scatter(partial_value, "row", scatter_dimension=0, tiled=True)
    first_row = lax.axis_index("row") * summed.shape[0]
    share_rows = summed.shape[0]
    by_trait = summed.reshape(share_rows, traits_here, set_count).transpose(0, 2, 1)
    by_trait = by_trait.reshape(share_rows, set_count * traits_here)
    grouped = lax.all_to_all(by_trait, "col", split_axis=1, concat_axis=1, tiled=True)
    grouped = grouped.reshape(share_rows, col_count, sets_dev, traits_here).transpose(0, 2, 1, 3)
    grouped = grouped.reshape(share_rows, sets_dev, traits)
    rotated = jnp.einsum("rst,tj->rsj", grouped, trait_basis, precision=HIGH)
    kin_rows = lax.dynamic_slice_in_dim(kin_values, first_row, share_rows, 0)
    product = kin_rows[:, None] * trait_values[None, :]
    scaled = rotated * (product / (product + 1.0))[:, None, :]
    unrotated = jnp.einsum("rsj,tj->rst", scaled, trait_basis, precision=HIGH)
    outgoing = unrotated.reshape(share_rows, sets_dev, col_count, traits_here).transpose(0, 2, 1, 3)
    outgoing = outgoing.reshape(share_rows, col_count * sets_dev * traits_here)
    returned = lax.all_to_all(outgoing, "col", split_axis=1, concat_axis=1, tiled=True)
    coeffs = returned.reshape(share_rows, set_count, traits_here).transpose(0, 2, 1)
    coeffs = coeffs.reshape(share_rows, columns)
    coeffs_low = lax.all_gather(coeffs.astype(jnp.bfloat16), "row", axis=0, tiled=True)
    genetic = jnp.dot(whole_panel, coeffs_low, preferred_element_type=jnp.float32)
    return (coeffs, genetic.astype(jnp.bfloat16))


def solution(mesh):
    return jax.shard_map(
        local,
        mesh=mesh,
        in_specs=(P("row", "col"), P("row", "col"), P(), P(), P()),
        out_specs=(P("row", "col"), P("row", "col")),
        check_vma=False,
    )
```

```python
import functools

import jax
import jax.numpy as jnp
from jax import lax
from jax.experimental import pallas as pl
from jax.experimental.pallas import tpu as pltpu
from jax.sharding import PartitionSpec as P

LANES = 128
PIECES = 8
EARLY = (0, 1, 2, 3, 4, 5)
LATE = (6, 7)
FROM_END = (1, 2, 3, 4, 5)
MID_FEED = 2
UNITS = 4
END_STEPS = (
    ("P10", "P11"),
    ("P20", "T00", "P21", "T01"),
    ("P22", "T02"),
    ("T03", "P23", "P30", "T10", "T11", "P31", "T20"),
    ("P32", "P33", "T21", "T22", "T23"),
    ("T30", "T31", "T32", "T33", "B12", "B13"),
)
MID_STEPS = (
    ("O10", "O11", "O20", "O21", "O22"),
    ("O23", "O30"),
    ("O31", "O32"),
    ("O33", "O12", "O13"),
    ("X12", "X13"),
    (),
)
TILES = 16
AHEAD = 8
MESH = pl.DeviceIdType.MESH
HIGH = lax.Precision.HIGHEST


def gather_rotate(
    rows, cols, q, pheno, basis_in, kin_in, trait_in,
    w_out, c_out, held,
    basis, kin, trait, g, ph, lent, acc, lent_acc, part_f, part, rparts, sb, rb, ob, crow, ct,
    load_sem, bulk_send, recv_sem, lend_recv, small_send, rs_recv, trade_recv, ag_recv,
):
    me_r, me_c = lax.axis_index("row"), lax.axis_index("col")
    lines = cols // 2
    z, y = me_c // 2, lax.rem(me_c, 2)
    width, people = q.shape
    piece = people // PIECES
    columns = pheno.shape[1]
    traits = basis.shape[0]
    sets = columns * cols // traits
    t_here = traits // cols
    late = people * len(LATE) // PIECES
    lot = late // PIECES

    own_load = pltpu.make_async_copy(q, g.at[me_c], load_sem.at[0])
    own_load.start()
    ph_load = pltpu.make_async_copy(pheno, ph, load_sem.at[1])
    ph_load.start()
    small = [
        pltpu.make_async_copy(a, b, load_sem.at[2 + i])
        for i, (a, b) in enumerate(((basis_in, basis), (kin_in, kin), (trait_in, trait)))
    ]
    for copy in small:
        copy.start()

    far = z // (lines // 2)
    place_of = lambda k: k + far * (lines - 1 - 2 * k)
    is_end = z == place_of(0)
    is_mid = jnp.logical_not(is_end)
    own = lambda k: 2 * place_of(k) + y

    barrier = pltpu.get_barrier_semaphore()

    def greet(r, c):
        pl.semaphore_signal(barrier, inc=1, device_id=(r, c), device_id_type=MESH)

    for d in range(1, rows):
        greet(lax.rem(me_r + d, rows), me_c)
    greet(me_r, me_c + 1 - 2 * y)

    @pl.when(is_end)
    def _():
        greet(me_r, own(1))
        pl.semaphore_wait(barrier, rows + 1)

    @pl.when(is_mid)
    def _():
        greet(me_r, own(0))
        greet(me_r, own(2))
        pl.semaphore_wait(barrier, rows + 2)

    across = lambda k: 2 * place_of(k) + 1 - y
    SAME, OTHER = own, across


    def bank(way):
        return 0 if way in (0, 1) else 1

    def sends_done(counts):
        for i, count in enumerate(counts):
            rows_of = w_out.at[pl.ds(0, int(count * width * piece) // w_out.shape[1])]
            pltpu.make_async_copy(rows_of, rows_of, bulk_send.at[i]).wait()

    def hop(way, kind, k, j):
        block = kind(k)
        target = me_c + 1 - 2 * y if way == "y" else own(way)
        here = g.at[block, :, pl.ds(j * piece, piece)]
        return pltpu.make_async_remote_copy(
            src_ref=here, dst_ref=here,
            send_sem=bulk_send.at[bank(way)], recv_sem=recv_sem.at[block, j],
            device_id=(me_r, target), device_id_type=MESH,
        )

    def lend(i):
        return pltpu.make_async_remote_copy(
            src_ref=pheno.at[pl.ds(people - late + i * lot, lot)], dst_ref=lent.at[pl.ds(i * lot, lot)],
            send_sem=bulk_send.at[0], recv_sem=lend_recv.at[i * len(LATE) // PIECES],
            device_id=(me_r, own(1)), device_id_type=MESH,
        )

    def lent_here(i):
        there = lent.at[pl.ds(i * piece, piece)]
        pltpu.make_async_copy(there, there, lend_recv.at[i]).wait()

    def sender(role):
        def send(way, kind, k, j):
            role.append((way, kind, k, j))
            hop(way, kind, k, j).start()

        return send

    def arrived(kind, k, j):
        hop("y", kind, k, j).wait_recv()

    def lhs_of(k, at):
        pair = place_of(k)
        return pair, at, jnp.concatenate([g[2 * pair, :, at], g[2 * pair + 1, :, at]], axis=0)

    def turn(pair, at, lhs):
        w_out[at, pl.ds(pl.multiple_of(pair * LANES, LANES), LANES)] = lhs.T

    def process(k, j):
        pair, at, lhs = lhs_of(k, pl.ds(j * piece, piece))
        acc[pair] += jnp.dot(lhs, ph[at, :], preferred_element_type=jnp.float32)
        turn(pair, at, lhs)

    def process_lent(k, j):
        pair, _, lhs = lhs_of(k, pl.ds(j * piece, piece))
        theirs = lent[pl.ds((j - LATE[0]) * piece, piece), :]
        lent_acc[pair] += jnp.dot(lhs, theirs, preferred_element_type=jnp.float32)

    def reduce_copy(pair, h):
        return pltpu.make_async_remote_copy(
            src_ref=part.at[h, pair], dst_ref=rparts.at[h, me_r],
            send_sem=small_send.at[h], recv_sem=rs_recv.at[h],
            device_id=(pair, me_c), device_id_type=MESH,
        )

    def finish_pair(k, h=0):
        pair = place_of(k)

        @pl.when(pair != me_r)
        def _():
            part[h, pair] = (lent_acc if h else acc)[pair].astype(jnp.bfloat16)
            reduce_copy(pair, h).start()

    def unit(u):
        size = late // UNITS
        return pl.ds(people - late + u * size, size)

    def late_hop(way, kind, k, u):
        block = kind(k)
        here = g.at[block, :, unit(u)]
        return pltpu.make_async_remote_copy(
            src_ref=here, dst_ref=here, send_sem=bulk_send.at[0], recv_sem=recv_sem.at[block, len(EARLY) + u],
            device_id=(me_r, me_c + 1 - 2 * y if way == "y" else own(way)), device_id_type=MESH,
        )

    late_sent = {"end": [], "mid": []}

    def late_send_off(role, way, kind, k, u):
        late_sent[role].append((way, kind, k, u))
        late_hop(way, kind, k, u).start()

    def late_steps(role, i):
        for what, k, u in (END_STEPS if role == "end" else MID_STEPS)[i]:
            k, u = int(k), int(u)
            if what == "P":
                late_hop("y", SAME, k, u).wait_recv()
                late_send_off(role, "y", SAME, k, u)
            elif what in "OX":
                late_send_off(role, 0, SAME if what == "O" else OTHER, k, u)
            else:
                if what == "B":
                    late_hop("y", SAME, k, u).wait_recv()
                late_hop("y", OTHER, k, u).wait_recv()
                turn(*lhs_of(k, unit(u)))

    acc[...] = jnp.zeros_like(acc)
    own_load.wait()
    end_sent, mid_sent = [], []

    @pl.when(is_end)
    def _():
        send = sender(end_sent)
        for j in range(PIECES):
            send(1, SAME, 0, j)
            if j in EARLY:
                send("y", SAME, 0, j)
        for i in range(PIECES):
            lend(i).start()
        ph_load.wait()
        n = len(EARLY)
        h = n // 2
        for t in range(3 * n):
            line, j = t // n, t % n
            arrived(SAME, 1 + line, j)
            if line or j < h:
                send("y", SAME, 1 + line, j)
            if line == 0:
                arrived(OTHER, 0, j)
                if j in FROM_END:
                    send(1, OTHER, 0, j)
                process(0, j)
            elif t < n + h:
                arrived(OTHER, 1, j)
                process(1, j)
            elif t < 2 * n + h:
                arrived(OTHER, 2, t - n - h)
                process(2, t - n - h)
            else:
                arrived(OTHER, 3, t - 2 * n - h)
                process(3, t - 2 * n - h)
            if t == n - 1:
                finish_pair(0)
            if t == 2 * n + h - 1:
                finish_pair(2)
        for u in range(UNITS):
            late_send_off("end", "y", SAME, 0, u)
        for j in range(h, n):
            arrived(OTHER, 1, j)
            process(1, j)
            if j == n - 1:
                finish_pair(1)
            arrived(OTHER, 3, j)
            process(3, j)
        finish_pair(3)
        late_steps("end", 0)

    @pl.when(is_mid)
    def _():
        send = sender(mid_sent)
        n = len(EARLY)
        for j in range(PIECES):
            if j in EARLY:
                send(0, SAME, 1, j)
                send(2, SAME, 1, j)
            send("y", SAME, 1, j)
        lent_acc[...] = jnp.zeros_like(lent_acc)
        ph_load.wait()
        for j in range(PIECES):
            arrived(SAME, 0, j)
            if j in EARLY:
                send(2, SAME, 0, j)
            if j not in FROM_END:
                send("y", SAME, 0, j)
            if j in EARLY:
                arrived(SAME, 2, j)
                send(0, SAME, 2, j)
                if j not in FROM_END:
                    send("y", SAME, 2, j)
            if j == n - 1:
                for i in LATE:
                    send(2, SAME, 1, i)
            if j in LATE:
                send(2, SAME, 0, j)
                arrived(SAME, 3, j - n)
                send(0, SAME, 3, j - n)
                send("y", SAME, 3, j - n)
            arrived(OTHER, 1, j)
            process(1, j)
        for j in FROM_END:
            send(2, OTHER, 1, j)
        finish_pair(1)
        first = [j for j in range(PIECES) if j not in FROM_END]
        b = len(LATE)
        early_y = EARLY[: n // 2]
        for i, (k, j) in enumerate([(0, first[0]), (2, first[0]), (0, LATE[0]), (3, early_y[0])]):
            arrived(SAME, 3, b + i)
            send(0, SAME, 3, b + i)
            if b + i in early_y:
                send("y", SAME, 3, b + i)
            arrived(OTHER, k, j)
            process(k, j)
        for j in EARLY[n // 2:]:
            send(0, OTHER, 1, j)
        lent_here(0)
        for k in (0, 1):
            process_lent(k, LATE[0])
        here = [(2, j) for j in LATE] + [(3, j) for j in LATE]
        for (k, j), (m, i) in zip(here, [(0, LATE[1]), (3, early_y[1]), (3, early_y[2]), (2, LATE[0])]):
            arrived(SAME, k, j)
            send("y", SAME, k, j)
            arrived(OTHER, m, i)
            process(m, i)
        for j in EARLY[n // 2:]:
            send("y", SAME, 3, j)
        lent_here(1)
        for k in (0, 1):
            process_lent(k, LATE[1])
            finish_pair(k, 1)
        process_lent(2, LATE[0])
        rest = [(2, LATE[1]), (3, LATE[0]), (3, LATE[1])] + [(3, j) for j in EARLY[n // 2:]]
        for i, j in enumerate(FROM_END):
            arrived(OTHER, 0, j)
            process(0, j)
            arrived(OTHER, 2, j)
            process(2, j)
            k, m = rest.pop(0)
            arrived(OTHER, k, m)
            process(k, m)
            if m in LATE:
                process_lent(k, m)
            if m == LATE[1]:
                finish_pair(k, 1)
            if i == MID_FEED:
                late_steps("mid", 0)
        finish_pair(0)
        finish_pair(2)
        for k, m in rest:
            arrived(OTHER, k, m)
            process(k, m)
        finish_pair(3)

    def exchange_time(i):
        @pl.when(is_end)
        def _():
            late_steps("end", i)

        @pl.when(is_mid)
        def _():
            late_steps("mid", i)

    def all_but_one(ref, sem):
        some = ref.at[pl.ds(0, ref.shape[0] - 1)]
        pltpu.make_async_copy(some, some, sem).wait()

    def total_of(h):
        all_but_one(rparts.at[h], rs_recv.at[h])
        total = (lent_acc if h else acc)[me_r]
        for d in range(1, rows):
            total = total + rparts[h, lax.rem(me_r + d, rows)].astype(jnp.float32)
        part_f[...] = total.T
        by_set = [part_f[pl.ds(s, t_here, stride=sets), :] for s in range(sets)]
        turned = jnp.concatenate(by_set, axis=0).astype(jnp.bfloat16)
        sb[:, h] = turned.reshape(cols, columns // cols, LANES)

    total_of(0)

    @pl.when(is_mid)
    def _():
        total_of(1)

    @pl.when(is_end)
    def _():
        sb[:, 1] = jnp.zeros_like(sb[:, 1])

    def trade1(peer, slot):
        return pltpu.make_async_remote_copy(
            src_ref=sb.at[peer], dst_ref=rb.at[slot], send_sem=small_send.at[2], recv_sem=trade_recv.at[0],
            device_id=(me_r, peer), device_id_type=MESH,
        )

    def trade2(peer, slot):
        return pltpu.make_async_remote_copy(
            src_ref=ob.at[peer], dst_ref=crow.at[me_r, slot], send_sem=small_send.at[3], recv_sem=trade_recv.at[1],
            device_id=(me_r, peer), device_id_type=MESH,
        )

    def share(peer, slot):
        return pltpu.make_async_remote_copy(
            src_ref=crow.at[me_r], dst_ref=crow.at[slot], send_sem=small_send.at[4], recv_sem=ag_recv.at[slot],
            device_id=(peer, me_c), device_id_type=MESH,
        )

    col_peers = [lax.rem(me_c + d, cols) for d in range(1, cols)]
    row_peers = [lax.rem(me_r + d, rows) for d in range(1, rows)]
    for p in col_peers:
        trade1(p, me_c).start()
    exchange_time(1)
    exchange_time(2)
    rb[me_c] = sb[me_c]
    for copy in small:
        copy.wait()
    product = kin[pl.ds(me_r, 1), :] * jnp.broadcast_to(trait[...], (LANES, traits)).T
    weight = product / (product + 1.0)
    all_but_one(rb, trade_recv.at[0])
    s_here = sets // cols

    def gathered(s):
        at = slice(s * t_here, (s + 1) * t_here)
        terms = []
        for c in range(cols):
            term = rb[c, 0, at, :].astype(jnp.float32)
            if c // 2 in (0, lines - 1):
                term = term + rb[c + 2 if c // 2 == 0 else c - 2, 1, at, :].astype(jnp.float32)
            terms.append(term)
        return jnp.concatenate(terms, axis=0)

    got = jnp.concatenate([gathered(s) for s in range(s_here)], axis=1)
    rotated = jnp.dot(basis[...].T, got, precision=HIGH, preferred_element_type=jnp.float32)
    scaled = rotated * jnp.concatenate([weight] * s_here, axis=1)
    back = jnp.dot(basis[...], scaled, precision=HIGH, preferred_element_type=jnp.float32)
    for s in range(s_here):
        ob[:, s * t_here:(s + 1) * t_here, :] = (
            back[:, s * LANES:(s + 1) * LANES].reshape(cols, t_here, LANES).astype(jnp.bfloat16)
        )
    for p in col_peers:
        trade2(p, me_c).start()
    exchange_time(3)
    crow[me_r, me_c] = ob[me_c]
    all_but_one(ob, trade_recv.at[1])
    for p in row_peers:
        share(p, me_r).start()

    def place(r):
        for s in range(sets):
            part_s = crow[r, s // s_here, (s % s_here) * t_here:(s % s_here + 1) * t_here, :]
            ct[pl.ds(s, t_here, stride=sets), :] = part_s.astype(jnp.float32)
        c_out[pl.ds(pl.multiple_of(r * LANES, LANES), LANES), :] = ct[...].T.astype(jnp.bfloat16)

    place(me_r)
    exchange_time(4)
    for p in row_peers:
        share(p, p).wait_recv()
        place(p)
    size = people // TILES
    for i in range(held.shape[0] // size):
        held[i * size:(i + 1) * size, :] = tile_of(w_out, c_out, i * size, size)
    exchange_time(5)

    def count(sent, others, late):
        counts = [others + late * piece_of_unit, 0]
        for way, *_ in sent:
            counts[bank(way)] += 1
        return counts

    piece_of_unit = late / (UNITS * piece)

    @pl.when(is_end)
    def _():
        sends_done(count(end_sent, PIECES, len(late_sent["end"])))

    @pl.when(is_mid)
    def _():
        sends_done(count(mid_sent, 0, len(late_sent["mid"])))
        all_but_one(part.at[1], small_send.at[1])

    all_but_one(part.at[0], small_send.at[0])
    all_but_one(sb, small_send.at[2])
    all_but_one(ob, small_send.at[3])
    all_but_one(crow, small_send.at[4])


def tile_of(w, c, first, size):
    return jnp.dot(w[first:first + size, :], c[...], preferred_element_type=jnp.float32).astype(jnp.bfloat16)


def predict(w, c, ready, gen_out, coeffs_out, held, coeffs, gen_sem):
    share = coeffs.shape[0]
    size = w.shape[0] // TILES
    done = ready.shape[0]
    copies = [pltpu.make_async_copy(ready, gen_out.at[pl.ds(0, done)], gen_sem.at[0])]
    copies[0].start()
    for i in range(done // size, TILES):
        at = pl.ds(i * size, size)
        held[at, :] = tile_of(w, c, i * size, size)
        copies.append(pltpu.make_async_copy(held.at[at], gen_out.at[at], gen_sem.at[i]))
        copies[-1].start()
        if i == done // size:
            mine = pl.ds(pl.multiple_of(lax.axis_index("row") * share, share), share)
            coeffs[...] = c[mine, :].astype(jnp.float32)
            copies.append(pltpu.make_async_copy(coeffs, coeffs_out, gen_sem.at[TILES]))
            copies[-1].start()
    for copy in copies:
        copy.wait()


def fused(panel, pheno, kin_values, trait_values, trait_basis):
    rows, cols = lax.axis_size("row"), lax.axis_size("col")
    ind, columns = pheno.shape
    traits = trait_basis.shape[0]
    sets = columns * cols // traits
    share = kin_values.shape[0] // rows
    bf, f32 = jnp.bfloat16, jnp.float32
    hbm = pl.BlockSpec(memory_space=pltpu.HBM)
    vmem = pl.BlockSpec(memory_space=pltpu.VMEM)
    lot = columns // cols
    dma = pltpu.SemaphoreType.DMA
    given = (panel.T, pheno, trait_basis, kin_values.reshape(rows, share), trait_values[None, :])
    whole, low, ready = pl.pallas_call(
        functools.partial(gather_rotate, rows, cols),
        out_shape=(
            pltpu.VMEM((ind, rows * share), bf),
            pltpu.VMEM((rows * share, columns), bf),
            pltpu.VMEM((ind * AHEAD // TILES, columns), bf),
        ),
        in_specs=[hbm] * 5,
        out_specs=(vmem, vmem, vmem),
        scratch_shapes=[
            pltpu.VMEM((traits, traits), f32),
            pltpu.VMEM((rows, share), f32),
            pltpu.VMEM((1, traits), f32),
            pltpu.VMEM((cols, panel.shape[1], ind), bf),
            pltpu.VMEM((ind, columns), bf),
            pltpu.VMEM((ind * len(LATE) // PIECES, columns), bf),
            pltpu.VMEM((rows, share, columns), f32),
            pltpu.VMEM((rows, share, columns), f32),
            pltpu.VMEM((columns, LANES), f32),
            pltpu.VMEM((2, rows, share, columns), bf),
            pltpu.VMEM((2, rows, share, columns), bf),
            pltpu.VMEM((cols, 2, lot, LANES), bf),
            pltpu.VMEM((cols, 2, lot, LANES), bf),
            pltpu.VMEM((cols, lot, LANES), bf),
            pltpu.VMEM((rows, cols, lot, LANES), bf),
            pltpu.VMEM((columns, LANES), f32),
            dma((5,)), dma((2,)), dma((cols, len(EARLY) + UNITS)), dma((len(LATE),)), dma((5,)), dma((2,)), dma((2,)), dma((rows,)),
        ],
        compiler_params=pltpu.CompilerParams(
            collective_id=0, has_side_effects=True, vmem_limit_bytes=36 * 1024 * 1024
        ),
    )(*(pltpu.with_memory_space_constraint(a, pltpu.HBM) for a in given))
    genetic, coeffs = pl.pallas_call(
        predict,
        out_shape=(
            jax.ShapeDtypeStruct((ind, columns), bf),
            jax.ShapeDtypeStruct((share, columns), f32),
        ),
        in_specs=[vmem] * 3,
        out_specs=(hbm, hbm),
        scratch_shapes=[pltpu.VMEM((ind, columns), bf), pltpu.VMEM((share, columns), f32), dma((TILES + 1,))],
        compiler_params=pltpu.CompilerParams(vmem_limit_bytes=20 * 1024 * 1024),
    )(whole, low, ready)
    return coeffs, genetic


def local(panel, pheno, kin_values, trait_values, trait_basis):
    rows, cols = lax.axis_size("row"), lax.axis_size("col")
    eigen = kin_values.shape[0]
    fits = 2 * panel.shape[1] == LANES and eigen // rows == LANES and trait_basis.shape[0] // cols == 16
    if fits and rows == 4 and cols == 2 * rows:
        return fused(panel, pheno, kin_values, trait_values, trait_basis)
    return plain(panel, pheno, kin_values, trait_values, trait_basis)


def plain(panel, pheno, kin_values, trait_values, trait_basis):
    col_count = lax.axis_size("col")
    columns = pheno.shape[1]
    traits = trait_basis.shape[0]
    traits_here = traits // col_count
    set_count = columns // traits_here
    sets_dev = set_count // col_count
    whole_panel = lax.all_gather(panel, "col", axis=1, tiled=True)
    partial_value = lax.dot_general(
        whole_panel, pheno, (((0,), (0,)), ((), ())), preferred_element_type=jnp.float32
    )
    summed = lax.psum_scatter(partial_value, "row", scatter_dimension=0, tiled=True)
    first_row = lax.axis_index("row") * summed.shape[0]
    share_rows = summed.shape[0]
    by_trait = summed.reshape(share_rows, traits_here, set_count).transpose(0, 2, 1)
    by_trait = by_trait.reshape(share_rows, set_count * traits_here)
    grouped = lax.all_to_all(by_trait, "col", split_axis=1, concat_axis=1, tiled=True)
    grouped = grouped.reshape(share_rows, col_count, sets_dev, traits_here).transpose(0, 2, 1, 3)
    grouped = grouped.reshape(share_rows, sets_dev, traits)
    rotated = jnp.einsum("rst,tj->rsj", grouped, trait_basis, precision=HIGH)
    kin_rows = lax.dynamic_slice_in_dim(kin_values, first_row, share_rows, 0)
    product = kin_rows[:, None] * trait_values[None, :]
    scaled = rotated * (product / (product + 1.0))[:, None, :]
    unrotated = jnp.einsum("rsj,tj->rst", scaled, trait_basis, precision=HIGH)
    outgoing = unrotated.reshape(share_rows, sets_dev, col_count, traits_here).transpose(0, 2, 1, 3)
    outgoing = outgoing.reshape(share_rows, col_count * sets_dev * traits_here)
    returned = lax.all_to_all(outgoing, "col", split_axis=1, concat_axis=1, tiled=True)
    coeffs = returned.reshape(share_rows, set_count, traits_here).transpose(0, 2, 1)
    coeffs = coeffs.reshape(share_rows, columns)
    coeffs_low = lax.all_gather(coeffs.astype(jnp.bfloat16), "row", axis=0, tiled=True)
    genetic = jnp.dot(whole_panel, coeffs_low, preferred_element_type=jnp.float32)
    return (coeffs, genetic.astype(jnp.bfloat16))


def solution(mesh):
    return jax.shard_map(
        local,
        mesh=mesh,
        in_specs=(P("row", "col"), P("row", "col"), P(), P(), P()),
        out_specs=(P("row", "col"), P("row", "col")),
        check_vma=False,
    )
```

```python
import functools

import jax
import jax.numpy as jnp
from jax import lax
from jax.experimental import pallas as pl
from jax.experimental.pallas import tpu as pltpu
from jax.sharding import PartitionSpec as P

LANES = 128
PIECES = 8
EARLY = (0, 1, 2, 3, 4, 5)
LATE = (6, 7)
FROM_END = (1, 2, 3, 4, 5)
MID_FEED = 2
UNITS = 4
END_STEPS = (
    ("P10", "P11"),
    ("P20", "T00", "P21", "T01"),
    ("P22", "T02", "P23"),
    ("P30", "T03", "P31", "P32", "T10", "T11", "T20"),
    ("P33", "T21", "T22", "T23", "T30", "T31"),
    ("T32", "T33", "B12", "B13"),
)
MID_STEPS = (
    ("O10", "O11", "O20", "O21", "O22"),
    ("O23", "O30"),
    ("O31", "O32"),
    ("O33", "O12", "O13"),
    ("X12", "X13"),
    (),
)
TILES = 16
AHEAD = 8
MESH = pl.DeviceIdType.MESH
HIGH = lax.Precision.HIGHEST


def gather_rotate(
    rows, cols, q, pheno, basis_in, kin_in, trait_in,
    w_out, c_out, held,
    basis, kin, trait, g, ph, lent, acc, lent_acc, part_f, part, rparts, sb, rb, ob, crow, ct,
    load_sem, bulk_send, recv_sem, lend_recv, small_send, rs_recv, trade_recv, ag_recv,
):
    me_r, me_c = lax.axis_index("row"), lax.axis_index("col")
    lines = cols // 2
    z, y = me_c // 2, lax.rem(me_c, 2)
    width, people = q.shape
    piece = people // PIECES
    columns = pheno.shape[1]
    traits = basis.shape[0]
    sets = columns * cols // traits
    t_here = traits // cols
    late = people * len(LATE) // PIECES
    lot = late // PIECES

    own_load = pltpu.make_async_copy(q, g.at[me_c], load_sem.at[0])
    own_load.start()
    ph_load = pltpu.make_async_copy(pheno, ph, load_sem.at[1])
    ph_load.start()
    small = [
        pltpu.make_async_copy(a, b, load_sem.at[2 + i])
        for i, (a, b) in enumerate(((basis_in, basis), (kin_in, kin), (trait_in, trait)))
    ]
    for copy in small:
        copy.start()

    far = z // (lines // 2)
    place_of = lambda k: k + far * (lines - 1 - 2 * k)
    is_end = z == place_of(0)
    is_mid = jnp.logical_not(is_end)
    own = lambda k: 2 * place_of(k) + y

    barrier = pltpu.get_barrier_semaphore()

    def greet(r, c):
        pl.semaphore_signal(barrier, inc=1, device_id=(r, c), device_id_type=MESH)

    for d in range(1, rows):
        greet(lax.rem(me_r + d, rows), me_c)
    greet(me_r, me_c + 1 - 2 * y)

    @pl.when(is_end)
    def _():
        greet(me_r, own(1))
        pl.semaphore_wait(barrier, rows + 1)

    @pl.when(is_mid)
    def _():
        greet(me_r, own(0))
        greet(me_r, own(2))
        pl.semaphore_wait(barrier, rows + 2)

    across = lambda k: 2 * place_of(k) + 1 - y
    SAME, OTHER = own, across


    def bank(way):
        return 0 if way in (0, 1) else 1

    def sends_done(counts):
        for i, count in enumerate(counts):
            rows_of = w_out.at[pl.ds(0, int(count * width * piece) // w_out.shape[1])]
            pltpu.make_async_copy(rows_of, rows_of, bulk_send.at[i]).wait()

    def hop(way, kind, k, j):
        block = kind(k)
        target = me_c + 1 - 2 * y if way == "y" else own(way)
        here = g.at[block, :, pl.ds(j * piece, piece)]
        return pltpu.make_async_remote_copy(
            src_ref=here, dst_ref=here,
            send_sem=bulk_send.at[bank(way)], recv_sem=recv_sem.at[block, j],
            device_id=(me_r, target), device_id_type=MESH,
        )

    def lend(i):
        return pltpu.make_async_remote_copy(
            src_ref=pheno.at[pl.ds(people - late + i * lot, lot)], dst_ref=lent.at[pl.ds(i * lot, lot)],
            send_sem=bulk_send.at[0], recv_sem=lend_recv.at[i * len(LATE) // PIECES],
            device_id=(me_r, own(1)), device_id_type=MESH,
        )

    def lent_here(i):
        there = lent.at[pl.ds(i * piece, piece)]
        pltpu.make_async_copy(there, there, lend_recv.at[i]).wait()

    def sender(role):
        def send(way, kind, k, j):
            role.append((way, kind, k, j))
            hop(way, kind, k, j).start()

        return send

    def arrived(kind, k, j):
        hop("y", kind, k, j).wait_recv()

    def lhs_of(k, at):
        pair = place_of(k)
        return pair, at, jnp.concatenate([g[2 * pair, :, at], g[2 * pair + 1, :, at]], axis=0)

    def turn(pair, at, lhs):
        w_out[at, pl.ds(pl.multiple_of(pair * LANES, LANES), LANES)] = lhs.T

    def process(k, j):
        pair, at, lhs = lhs_of(k, pl.ds(j * piece, piece))
        acc[pair] += jnp.dot(lhs, ph[at, :], preferred_element_type=jnp.float32)
        turn(pair, at, lhs)

    def process_lent(k, j):
        pair, _, lhs = lhs_of(k, pl.ds(j * piece, piece))
        theirs = lent[pl.ds((j - LATE[0]) * piece, piece), :]
        lent_acc[pair] += jnp.dot(lhs, theirs, preferred_element_type=jnp.float32)

    def reduce_copy(pair, h):
        return pltpu.make_async_remote_copy(
            src_ref=part.at[h, pair], dst_ref=rparts.at[h, me_r],
            send_sem=small_send.at[h], recv_sem=rs_recv.at[h],
            device_id=(pair, me_c), device_id_type=MESH,
        )

    def finish_pair(k, h=0):
        pair = place_of(k)

        @pl.when(pair != me_r)
        def _():
            part[h, pair] = (lent_acc if h else acc)[pair].astype(jnp.bfloat16)
            reduce_copy(pair, h).start()

    def unit(u):
        size = late // UNITS
        return pl.ds(people - late + u * size, size)

    def late_hop(way, kind, k, u):
        block = kind(k)
        here = g.at[block, :, unit(u)]
        return pltpu.make_async_remote_copy(
            src_ref=here, dst_ref=here, send_sem=bulk_send.at[0], recv_sem=recv_sem.at[block, len(EARLY) + u],
            device_id=(me_r, me_c + 1 - 2 * y if way == "y" else own(way)), device_id_type=MESH,
        )

    late_sent = {"end": [], "mid": []}

    def late_send_off(role, way, kind, k, u):
        late_sent[role].append((way, kind, k, u))
        late_hop(way, kind, k, u).start()

    def late_steps(role, i):
        for what, k, u in (END_STEPS if role == "end" else MID_STEPS)[i]:
            k, u = int(k), int(u)
            if what == "P":
                late_hop("y", SAME, k, u).wait_recv()
                late_send_off(role, "y", SAME, k, u)
            elif what in "OX":
                late_send_off(role, 0, SAME if what == "O" else OTHER, k, u)
            else:
                if what == "B":
                    late_hop("y", SAME, k, u).wait_recv()
                late_hop("y", OTHER, k, u).wait_recv()
                turn(*lhs_of(k, unit(u)))

    acc[...] = jnp.zeros_like(acc)
    own_load.wait()
    end_sent, mid_sent = [], []

    @pl.when(is_end)
    def _():
        send = sender(end_sent)
        for j in range(PIECES):
            send(1, SAME, 0, j)
            if j in EARLY:
                send("y", SAME, 0, j)
        for i in range(PIECES):
            lend(i).start()
        ph_load.wait()
        n = len(EARLY)
        h = n // 2
        for t in range(3 * n):
            line, j = t // n, t % n
            arrived(SAME, 1 + line, j)
            if line or j < h:
                send("y", SAME, 1 + line, j)
            if line == 0:
                arrived(OTHER, 0, j)
                if j in FROM_END:
                    send(1, OTHER, 0, j)
                process(0, j)
            elif t < n + h:
                arrived(OTHER, 1, j)
                process(1, j)
            elif t < 2 * n + h:
                arrived(OTHER, 2, t - n - h)
                process(2, t - n - h)
            else:
                arrived(OTHER, 3, t - 2 * n - h)
                process(3, t - 2 * n - h)
            if t == n - 1:
                finish_pair(0)
            if t == 2 * n + h - 1:
                finish_pair(2)
        for u in range(UNITS):
            late_send_off("end", "y", SAME, 0, u)
        for j in range(h, n):
            arrived(OTHER, 1, j)
            process(1, j)
            if j == n - 1:
                finish_pair(1)
            arrived(OTHER, 3, j)
            process(3, j)
        finish_pair(3)
        late_steps("end", 0)

    @pl.when(is_mid)
    def _():
        send = sender(mid_sent)
        n = len(EARLY)
        for j in range(PIECES):
            if j in EARLY:
                send(0, SAME, 1, j)
                send(2, SAME, 1, j)
            send("y", SAME, 1, j)
        lent_acc[...] = jnp.zeros_like(lent_acc)
        ph_load.wait()
        for j in range(PIECES):
            arrived(SAME, 0, j)
            if j in EARLY:
                send(2, SAME, 0, j)
            if j not in FROM_END:
                send("y", SAME, 0, j)
            if j in EARLY:
                arrived(SAME, 2, j)
                send(0, SAME, 2, j)
                if j not in FROM_END:
                    send("y", SAME, 2, j)
            if j == n - 1:
                for i in LATE:
                    send(2, SAME, 1, i)
            if j in LATE:
                send(2, SAME, 0, j)
                arrived(SAME, 3, j - n)
                send(0, SAME, 3, j - n)
                send("y", SAME, 3, j - n)
            arrived(OTHER, 1, j)
            process(1, j)
        for j in FROM_END:
            send(2, OTHER, 1, j)
        finish_pair(1)
        first = [j for j in range(PIECES) if j not in FROM_END]
        b = len(LATE)
        early_y = EARLY[: n // 2]
        for i, (k, j) in enumerate([(0, first[0]), (2, first[0]), (0, LATE[0]), (3, early_y[0])]):
            arrived(SAME, 3, b + i)
            send(0, SAME, 3, b + i)
            if b + i in early_y:
                send("y", SAME, 3, b + i)
            arrived(OTHER, k, j)
            process(k, j)
        for j in EARLY[n // 2:]:
            send(0, OTHER, 1, j)
        lent_here(0)
        for k in (0, 1):
            process_lent(k, LATE[0])
        here = [(2, j) for j in LATE] + [(3, j) for j in LATE]
        for (k, j), (m, i) in zip(here, [(0, LATE[1]), (3, early_y[1]), (3, early_y[2]), (2, LATE[0])]):
            arrived(SAME, k, j)
            send("y", SAME, k, j)
            arrived(OTHER, m, i)
            process(m, i)
        for j in EARLY[n // 2:]:
            send("y", SAME, 3, j)
        lent_here(1)
        for k in (0, 1):
            process_lent(k, LATE[1])
            finish_pair(k, 1)
        process_lent(2, LATE[0])
        rest = [(2, LATE[1]), (3, LATE[0]), (3, LATE[1])] + [(3, j) for j in EARLY[n // 2:]]
        for i, j in enumerate(FROM_END):
            arrived(OTHER, 0, j)
            process(0, j)
            arrived(OTHER, 2, j)
            process(2, j)
            k, m = rest.pop(0)
            arrived(OTHER, k, m)
            process(k, m)
            if m in LATE:
                process_lent(k, m)
            if m == LATE[1]:
                finish_pair(k, 1)
            if i == MID_FEED:
                late_steps("mid", 0)
        finish_pair(0)
        finish_pair(2)
        for k, m in rest:
            arrived(OTHER, k, m)
            process(k, m)
        finish_pair(3)

    def exchange_time(i):
        @pl.when(is_end)
        def _():
            late_steps("end", i)

        @pl.when(is_mid)
        def _():
            late_steps("mid", i)

    def all_but_one(ref, sem):
        some = ref.at[pl.ds(0, ref.shape[0] - 1)]
        pltpu.make_async_copy(some, some, sem).wait()

    def total_of(h):
        all_but_one(rparts.at[h], rs_recv.at[h])
        total = (lent_acc if h else acc)[me_r]
        for d in range(1, rows):
            total = total + rparts[h, lax.rem(me_r + d, rows)].astype(jnp.float32)
        part_f[...] = total.T
        by_set = [part_f[pl.ds(s, t_here, stride=sets), :] for s in range(sets)]
        turned = jnp.concatenate(by_set, axis=0).astype(jnp.bfloat16)
        sb[h] = turned.reshape(cols, columns // cols, LANES)

    total_of(0)

    @pl.when(is_mid)
    def _():
        total_of(1)

    def trade1(peer, slot, h):
        return pltpu.make_async_remote_copy(
            src_ref=sb.at[h, peer], dst_ref=rb.at[h, slot],
            send_sem=small_send.at[(2, 5)[h]], recv_sem=trade_recv.at[(0, 2)[h]],
            device_id=(me_r, peer), device_id_type=MESH,
        )

    def trade2(peer, slot):
        return pltpu.make_async_remote_copy(
            src_ref=ob.at[peer], dst_ref=crow.at[me_r, slot], send_sem=small_send.at[3], recv_sem=trade_recv.at[1],
            device_id=(me_r, peer), device_id_type=MESH,
        )

    def share(peer, slot):
        return pltpu.make_async_remote_copy(
            src_ref=crow.at[me_r], dst_ref=crow.at[slot], send_sem=small_send.at[4], recv_sem=ag_recv.at[slot],
            device_id=(peer, me_c), device_id_type=MESH,
        )

    col_peers = [lax.rem(me_c + d, cols) for d in range(1, cols)]
    row_peers = [lax.rem(me_r + d, rows) for d in range(1, rows)]
    for p in col_peers:
        trade1(p, me_c, 0).start()

    @pl.when(is_mid)
    def _():
        for p in col_peers:
            trade1(p, me_c, 1).start()
        rb[1, me_c] = sb[1, me_c]

    exchange_time(1)
    exchange_time(2)
    rb[0, me_c] = sb[0, me_c]
    for copy in small:
        copy.wait()
    product = kin[pl.ds(me_r, 1), :] * jnp.broadcast_to(trait[...], (LANES, traits)).T
    weight = product / (product + 1.0)
    all_but_one(rb.at[0], trade_recv.at[0])
    for role, senders in ((is_end, cols - 4), (is_mid, cols - 5)):

        @pl.when(role)
        def _():
            some = rb.at[1, pl.ds(0, senders)]
            pltpu.make_async_copy(some, some, trade_recv.at[2]).wait()

    s_here = sets // cols

    def gathered(s):
        at = slice(s * t_here, (s + 1) * t_here)
        terms = []
        for c in range(cols):
            term = rb[0, c, at, :].astype(jnp.float32)
            if c // 2 in (0, lines - 1):
                term = term + rb[1, c + 2 if c // 2 == 0 else c - 2, at, :].astype(jnp.float32)
            terms.append(term)
        return jnp.concatenate(terms, axis=0)

    got = jnp.concatenate([gathered(s) for s in range(s_here)], axis=1)
    rotated = jnp.dot(basis[...].T, got, precision=HIGH, preferred_element_type=jnp.float32)
    scaled = rotated * jnp.concatenate([weight] * s_here, axis=1)
    back = jnp.dot(basis[...], scaled, precision=HIGH, preferred_element_type=jnp.float32)
    for s in range(s_here):
        ob[:, s * t_here:(s + 1) * t_here, :] = (
            back[:, s * LANES:(s + 1) * LANES].reshape(cols, t_here, LANES).astype(jnp.bfloat16)
        )
    for p in col_peers:
        trade2(p, me_c).start()
    exchange_time(3)
    crow[me_r, me_c] = ob[me_c]
    all_but_one(ob, trade_recv.at[1])
    for p in row_peers:
        share(p, me_r).start()

    def place(r):
        for s in range(sets):
            part_s = crow[r, s // s_here, (s % s_here) * t_here:(s % s_here + 1) * t_here, :]
            ct[pl.ds(s, t_here, stride=sets), :] = part_s.astype(jnp.float32)
        c_out[pl.ds(pl.multiple_of(r * LANES, LANES), LANES), :] = ct[...].T.astype(jnp.bfloat16)

    place(me_r)
    exchange_time(4)
    for p in row_peers:
        share(p, p).wait_recv()
        place(p)
    size = people // TILES
    for i in range(held.shape[0] // size):
        held[i * size:(i + 1) * size, :] = tile_of(w_out, c_out, i * size, size)
    exchange_time(5)

    def count(sent, others, late):
        counts = [others + late * piece_of_unit, 0]
        for way, *_ in sent:
            counts[bank(way)] += 1
        return counts

    piece_of_unit = late / (UNITS * piece)

    @pl.when(is_end)
    def _():
        sends_done(count(end_sent, PIECES, len(late_sent["end"])))

    @pl.when(is_mid)
    def _():
        sends_done(count(mid_sent, 0, len(late_sent["mid"])))
        all_but_one(part.at[1], small_send.at[1])
        all_but_one(sb.at[1], small_send.at[5])

    all_but_one(part.at[0], small_send.at[0])
    all_but_one(sb.at[0], small_send.at[2])
    all_but_one(ob, small_send.at[3])
    all_but_one(crow, small_send.at[4])


def tile_of(w, c, first, size):
    return jnp.dot(w[first:first + size, :], c[...], preferred_element_type=jnp.float32).astype(jnp.bfloat16)


def predict(w, c, ready, gen_out, coeffs_out, held, coeffs, gen_sem):
    share = coeffs.shape[0]
    size = w.shape[0] // TILES
    done = ready.shape[0]
    copies = [pltpu.make_async_copy(ready, gen_out.at[pl.ds(0, done)], gen_sem.at[0])]
    copies[0].start()
    for i in range(done // size, TILES):
        at = pl.ds(i * size, size)
        held[at, :] = tile_of(w, c, i * size, size)
        copies.append(pltpu.make_async_copy(held.at[at], gen_out.at[at], gen_sem.at[i]))
        copies[-1].start()
        if i == done // size:
            mine = pl.ds(pl.multiple_of(lax.axis_index("row") * share, share), share)
            coeffs[...] = c[mine, :].astype(jnp.float32)
            copies.append(pltpu.make_async_copy(coeffs, coeffs_out, gen_sem.at[TILES]))
            copies[-1].start()
    for copy in copies:
        copy.wait()


def fused(panel, pheno, kin_values, trait_values, trait_basis):
    rows, cols = lax.axis_size("row"), lax.axis_size("col")
    ind, columns = pheno.shape
    traits = trait_basis.shape[0]
    sets = columns * cols // traits
    share = kin_values.shape[0] // rows
    bf, f32 = jnp.bfloat16, jnp.float32
    hbm = pl.BlockSpec(memory_space=pltpu.HBM)
    vmem = pl.BlockSpec(memory_space=pltpu.VMEM)
    lot = columns // cols
    dma = pltpu.SemaphoreType.DMA
    given = (panel.T, pheno, trait_basis, kin_values.reshape(rows, share), trait_values[None, :])
    whole, low, ready = pl.pallas_call(
        functools.partial(gather_rotate, rows, cols),
        out_shape=(
            pltpu.VMEM((ind, rows * share), bf),
            pltpu.VMEM((rows * share, columns), bf),
            pltpu.VMEM((ind * AHEAD // TILES, columns), bf),
        ),
        in_specs=[hbm] * 5,
        out_specs=(vmem, vmem, vmem),
        scratch_shapes=[
            pltpu.VMEM((traits, traits), f32),
            pltpu.VMEM((rows, share), f32),
            pltpu.VMEM((1, traits), f32),
            pltpu.VMEM((cols, panel.shape[1], ind), bf),
            pltpu.VMEM((ind, columns), bf),
            pltpu.VMEM((ind * len(LATE) // PIECES, columns), bf),
            pltpu.VMEM((rows, share, columns), f32),
            pltpu.VMEM((rows, share, columns), f32),
            pltpu.VMEM((columns, LANES), f32),
            pltpu.VMEM((2, rows, share, columns), bf),
            pltpu.VMEM((2, rows, share, columns), bf),
            pltpu.VMEM((2, cols, lot, LANES), bf),
            pltpu.VMEM((2, cols, lot, LANES), bf),
            pltpu.VMEM((cols, lot, LANES), bf),
            pltpu.VMEM((rows, cols, lot, LANES), bf),
            pltpu.VMEM((columns, LANES), f32),
            dma((5,)), dma((2,)), dma((cols, len(EARLY) + UNITS)), dma((len(LATE),)), dma((6,)), dma((2,)), dma((3,)), dma((rows,)),
        ],
        compiler_params=pltpu.CompilerParams(
            collective_id=0, has_side_effects=True, vmem_limit_bytes=36 * 1024 * 1024
        ),
    )(*(pltpu.with_memory_space_constraint(a, pltpu.HBM) for a in given))
    genetic, coeffs = pl.pallas_call(
        predict,
        out_shape=(
            jax.ShapeDtypeStruct((ind, columns), bf),
            jax.ShapeDtypeStruct((share, columns), f32),
        ),
        in_specs=[vmem] * 3,
        out_specs=(hbm, hbm),
        scratch_shapes=[pltpu.VMEM((ind, columns), bf), pltpu.VMEM((share, columns), f32), dma((TILES + 1,))],
        compiler_params=pltpu.CompilerParams(vmem_limit_bytes=20 * 1024 * 1024),
    )(whole, low, ready)
    return coeffs, genetic


def local(panel, pheno, kin_values, trait_values, trait_basis):
    rows, cols = lax.axis_size("row"), lax.axis_size("col")
    eigen = kin_values.shape[0]
    fits = 2 * panel.shape[1] == LANES and eigen // rows == LANES and trait_basis.shape[0] // cols == 16
    if fits and rows == 4 and cols == 2 * rows:
        return fused(panel, pheno, kin_values, trait_values, trait_basis)
    return plain(panel, pheno, kin_values, trait_values, trait_basis)


def plain(panel, pheno, kin_values, trait_values, trait_basis):
    col_count = lax.axis_size("col")
    columns = pheno.shape[1]
    traits = trait_basis.shape[0]
    traits_here = traits // col_count
    set_count = columns // traits_here
    sets_dev = set_count // col_count
    whole_panel = lax.all_gather(panel, "col", axis=1, tiled=True)
    partial_value = lax.dot_general(
        whole_panel, pheno, (((0,), (0,)), ((), ())), preferred_element_type=jnp.float32
    )
    summed = lax.psum_scatter(partial_value, "row", scatter_dimension=0, tiled=True)
    first_row = lax.axis_index("row") * summed.shape[0]
    share_rows = summed.shape[0]
    by_trait = summed.reshape(share_rows, traits_here, set_count).transpose(0, 2, 1)
    by_trait = by_trait.reshape(share_rows, set_count * traits_here)
    grouped = lax.all_to_all(by_trait, "col", split_axis=1, concat_axis=1, tiled=True)
    grouped = grouped.reshape(share_rows, col_count, sets_dev, traits_here).transpose(0, 2, 1, 3)
    grouped = grouped.reshape(share_rows, sets_dev, traits)
    rotated = jnp.einsum("rst,tj->rsj", grouped, trait_basis, precision=HIGH)
    kin_rows = lax.dynamic_slice_in_dim(kin_values, first_row, share_rows, 0)
    product = kin_rows[:, None] * trait_values[None, :]
    scaled = rotated * (product / (product + 1.0))[:, None, :]
    unrotated = jnp.einsum("rsj,tj->rst", scaled, trait_basis, precision=HIGH)
    outgoing = unrotated.reshape(share_rows, sets_dev, col_count, traits_here).transpose(0, 2, 1, 3)
    outgoing = outgoing.reshape(share_rows, col_count * sets_dev * traits_here)
    returned = lax.all_to_all(outgoing, "col", split_axis=1, concat_axis=1, tiled=True)
    coeffs = returned.reshape(share_rows, set_count, traits_here).transpose(0, 2, 1)
    coeffs = coeffs.reshape(share_rows, columns)
    coeffs_low = lax.all_gather(coeffs.astype(jnp.bfloat16), "row", axis=0, tiled=True)
    genetic = jnp.dot(whole_panel, coeffs_low, preferred_element_type=jnp.float32)
    return (coeffs, genetic.astype(jnp.bfloat16))


def solution(mesh):
    return jax.shard_map(
        local,
        mesh=mesh,
        in_specs=(P("row", "col"), P("row", "col"), P(), P(), P()),
        out_specs=(P("row", "col"), P("row", "col")),
        check_vma=False,
    )
```

```python
import functools

import jax
import jax.numpy as jnp
from jax import lax
from jax.experimental import pallas as pl
from jax.experimental.pallas import tpu as pltpu
from jax.sharding import PartitionSpec as P

LANES = 128
PIECES = 8
EARLY = (0, 1, 2, 3, 4, 5)
LATE = (6, 7)
FROM_END = (1, 2, 3, 4, 5)
MID_FEED = 2
UNITS = 4
END_STEPS = (
    ("P10", "P11"),
    ("P20", "T00", "P21", "T01"),
    ("P22", "T02", "P23"),
    ("P30", "T03", "P31", "P32", "T10", "T11", "T20"),
    ("P33", "T21", "T22", "T23", "T30", "T31"),
    ("T32", "T33", "B12", "B13"),
)
MID_STEPS = (
    ("O10", "O11", "O20", "O21", "O22"),
    ("O23", "O30"),
    ("O31", "O32"),
    ("O33", "O12", "O13"),
    ("X12", "X13"),
    (),
)
TILES = 16
AHEAD = 8
MESH = pl.DeviceIdType.MESH
HIGH = lax.Precision.HIGHEST


def gather_rotate(
    rows, cols, q, pheno, basis_in, kin_in, trait_in,
    w_out, c_out, held,
    basis, kin, trait, g, ph, lent, acc, lent_acc, part_f, part, rparts, sb, rb, ob, crow, ct,
    load_sem, bulk_send, recv_sem, lend_recv, small_send, rs_recv, trade_recv, ag_recv,
):
    me_r, me_c = lax.axis_index("row"), lax.axis_index("col")
    lines = cols // 2
    z, y = me_c // 2, lax.rem(me_c, 2)
    width, people = q.shape
    piece = people // PIECES
    columns = pheno.shape[1]
    traits = basis.shape[0]
    sets = columns * cols // traits
    t_here = traits // cols
    late = people * len(LATE) // PIECES
    lot = late // PIECES

    own_load = pltpu.make_async_copy(q, g.at[me_c], load_sem.at[0])
    own_load.start()
    ph_load = pltpu.make_async_copy(pheno, ph, load_sem.at[1])
    ph_load.start()
    small = [
        pltpu.make_async_copy(a, b, load_sem.at[2 + i])
        for i, (a, b) in enumerate(((basis_in, basis), (kin_in, kin), (trait_in, trait)))
    ]
    for copy in small:
        copy.start()

    far = z // (lines // 2)
    place_of = lambda k: k + far * (lines - 1 - 2 * k)
    is_end = z == place_of(0)
    is_mid = jnp.logical_not(is_end)
    own = lambda k: 2 * place_of(k) + y

    barrier = pltpu.get_barrier_semaphore()

    def greet(r, c):
        pl.semaphore_signal(barrier, inc=1, device_id=(r, c), device_id_type=MESH)

    for d in range(1, rows):
        greet(lax.rem(me_r + d, rows), me_c)
    greet(me_r, me_c + 1 - 2 * y)

    @pl.when(is_end)
    def _():
        greet(me_r, own(1))
        pl.semaphore_wait(barrier, rows + 1)

    @pl.when(is_mid)
    def _():
        greet(me_r, own(0))
        greet(me_r, own(2))
        pl.semaphore_wait(barrier, rows + 2)

    across = lambda k: 2 * place_of(k) + 1 - y
    SAME, OTHER = own, across


    def bank(way):
        return 0 if way in (0, 1) else 1

    def sends_done(counts):
        for i, count in enumerate(counts):
            rows_of = w_out.at[pl.ds(0, int(count * width * piece) // w_out.shape[1])]
            pltpu.make_async_copy(rows_of, rows_of, bulk_send.at[i]).wait()

    def hop(way, kind, k, j):
        block = kind(k)
        target = me_c + 1 - 2 * y if way == "y" else own(way)
        here = g.at[block, :, pl.ds(j * piece, piece)]
        return pltpu.make_async_remote_copy(
            src_ref=here, dst_ref=here,
            send_sem=bulk_send.at[bank(way)], recv_sem=recv_sem.at[block, j],
            device_id=(me_r, target), device_id_type=MESH,
        )

    def lend(i):
        return pltpu.make_async_remote_copy(
            src_ref=pheno.at[pl.ds(people - late + i * lot, lot)], dst_ref=lent.at[pl.ds(i * lot, lot)],
            send_sem=bulk_send.at[0], recv_sem=lend_recv.at[i * len(LATE) // PIECES],
            device_id=(me_r, own(1)), device_id_type=MESH,
        )

    def lent_here(i):
        there = lent.at[pl.ds(i * piece, piece)]
        pltpu.make_async_copy(there, there, lend_recv.at[i]).wait()

    def sender(role):
        def send(way, kind, k, j):
            role.append((way, kind, k, j))
            hop(way, kind, k, j).start()

        return send

    def arrived(kind, k, j):
        hop("y", kind, k, j).wait_recv()

    def lhs_of(k, at):
        pair = place_of(k)
        return pair, at, jnp.concatenate([g[2 * pair, :, at], g[2 * pair + 1, :, at]], axis=0)

    def turn(pair, at, lhs):
        w_out[at, pl.ds(pl.multiple_of(pair * LANES, LANES), LANES)] = lhs.T

    def process(k, j):
        pair, at, lhs = lhs_of(k, pl.ds(j * piece, piece))
        acc[pair] += jnp.dot(lhs, ph[at, :], preferred_element_type=jnp.float32)
        turn(pair, at, lhs)

    def process_lent(k, j):
        pair, _, lhs = lhs_of(k, pl.ds(j * piece, piece))
        theirs = lent[pl.ds((j - LATE[0]) * piece, piece), :]
        lent_acc[pair] += jnp.dot(lhs, theirs, preferred_element_type=jnp.float32)

    def reduce_copy(pair, h):
        return pltpu.make_async_remote_copy(
            src_ref=part.at[h, pair], dst_ref=rparts.at[h, me_r],
            send_sem=small_send.at[h], recv_sem=rs_recv.at[h],
            device_id=(pair, me_c), device_id_type=MESH,
        )

    def finish_pair(k, h=0):
        pair = place_of(k)

        @pl.when(pair != me_r)
        def _():
            part[h, pair] = (lent_acc if h else acc)[pair].astype(jnp.bfloat16)
            reduce_copy(pair, h).start()

    def unit(u):
        size = late // UNITS
        return pl.ds(people - late + u * size, size)

    def late_hop(way, kind, k, u):
        block = kind(k)
        here = g.at[block, :, unit(u)]
        return pltpu.make_async_remote_copy(
            src_ref=here, dst_ref=here, send_sem=bulk_send.at[0], recv_sem=recv_sem.at[block, len(EARLY) + u],
            device_id=(me_r, me_c + 1 - 2 * y if way == "y" else own(way)), device_id_type=MESH,
        )

    late_sent = {"end": [], "mid": []}

    def late_send_off(role, way, kind, k, u):
        late_sent[role].append((way, kind, k, u))
        late_hop(way, kind, k, u).start()

    def late_steps(role, i):
        for what, k, u in (END_STEPS if role == "end" else MID_STEPS)[i]:
            k, u = int(k), int(u)
            if what == "P":
                late_hop("y", SAME, k, u).wait_recv()
                late_send_off(role, "y", SAME, k, u)
            elif what in "OX":
                late_send_off(role, 0, SAME if what == "O" else OTHER, k, u)
            else:
                if what == "B":
                    late_hop("y", SAME, k, u).wait_recv()
                late_hop("y", OTHER, k, u).wait_recv()
                turn(*lhs_of(k, unit(u)))

    acc[...] = jnp.zeros_like(acc)
    own_load.wait()
    end_sent, mid_sent = [], []

    @pl.when(is_end)
    def _():
        send = sender(end_sent)
        for j in range(PIECES):
            send(1, SAME, 0, j)
            if j in EARLY:
                send("y", SAME, 0, j)
        for i in range(PIECES):
            lend(i).start()
        ph_load.wait()
        n = len(EARLY)
        h = n // 2
        for t in range(3 * n):
            line, j = t // n, t % n
            arrived(SAME, 1 + line, j)
            if line or j < h:
                send("y", SAME, 1 + line, j)
            if line == 0:
                arrived(OTHER, 0, j)
                if j in FROM_END:
                    send(1, OTHER, 0, j)
                process(0, j)
            elif t < n + h:
                arrived(OTHER, 1, j)
                process(1, j)
            elif t < 2 * n + h:
                arrived(OTHER, 2, t - n - h)
                process(2, t - n - h)
            else:
                arrived(OTHER, 3, t - 2 * n - h)
                process(3, t - 2 * n - h)
            if t == n - 1:
                finish_pair(0)
            if t == 2 * n + h - 1:
                finish_pair(2)
        for u in range(UNITS):
            late_send_off("end", "y", SAME, 0, u)
        for j in range(h, n):
            arrived(OTHER, 1, j)
            process(1, j)
            if j == n - 1:
                finish_pair(1)
            arrived(OTHER, 3, j)
            process(3, j)
        finish_pair(3)
        late_steps("end", 0)

    @pl.when(is_mid)
    def _():
        send = sender(mid_sent)
        n = len(EARLY)
        for j in range(PIECES):
            if j in EARLY:
                send(0, SAME, 1, j)
                send(2, SAME, 1, j)
            send("y", SAME, 1, j)
        lent_acc[...] = jnp.zeros_like(lent_acc)
        ph_load.wait()
        for j in range(PIECES):
            arrived(SAME, 0, j)
            if j in EARLY:
                send(2, SAME, 0, j)
            if j not in FROM_END:
                send("y", SAME, 0, j)
            if j in EARLY:
                arrived(SAME, 2, j)
                send(0, SAME, 2, j)
                if j not in FROM_END:
                    send("y", SAME, 2, j)
            if j == n - 1:
                for i in LATE:
                    send(2, SAME, 1, i)
            if j in LATE:
                send(2, SAME, 0, j)
                arrived(SAME, 3, j - n)
                send(0, SAME, 3, j - n)
                send("y", SAME, 3, j - n)
            arrived(OTHER, 1, j)
            process(1, j)
        for j in FROM_END:
            send(2, OTHER, 1, j)
        finish_pair(1)
        first = [j for j in range(PIECES) if j not in FROM_END]
        b = len(LATE)
        early_y = EARLY[: n // 2]
        for i, (k, j) in enumerate([(0, first[0]), (2, first[0]), (0, LATE[0]), (3, early_y[0])]):
            arrived(SAME, 3, b + i)
            send(0, SAME, 3, b + i)
            if b + i in early_y:
                send("y", SAME, 3, b + i)
            arrived(OTHER, k, j)
            process(k, j)
        for j in EARLY[n // 2:]:
            send(0, OTHER, 1, j)
        lent_here(0)
        for k in (0, 1):
            process_lent(k, LATE[0])
        here = [(2, j) for j in LATE] + [(3, j) for j in LATE]
        for (k, j), (m, i) in zip(here, [(0, LATE[1]), (3, early_y[1]), (3, early_y[2]), (2, LATE[0])]):
            arrived(SAME, k, j)
            send("y", SAME, k, j)
            arrived(OTHER, m, i)
            process(m, i)
        for j in EARLY[n // 2:]:
            send("y", SAME, 3, j)
        lent_here(1)
        for k in (0, 1):
            process_lent(k, LATE[1])
            finish_pair(k, 1)
        process_lent(2, LATE[0])
        rest = [(2, LATE[1]), (3, LATE[0]), (3, LATE[1])] + [(3, j) for j in EARLY[n // 2:]]
        for i, j in enumerate(FROM_END):
            arrived(OTHER, 0, j)
            process(0, j)
            arrived(OTHER, 2, j)
            process(2, j)
            k, m = rest.pop(0)
            arrived(OTHER, k, m)
            process(k, m)
            if m in LATE:
                process_lent(k, m)
            if m == LATE[1]:
                finish_pair(k, 1)
            if i == MID_FEED:
                late_steps("mid", 0)
        finish_pair(0)
        finish_pair(2)
        for k, m in rest:
            arrived(OTHER, k, m)
            process(k, m)
        finish_pair(3)

    def exchange_time(i):
        @pl.when(is_end)
        def _():
            late_steps("end", i)

        @pl.when(is_mid)
        def _():
            late_steps("mid", i)

    def all_but_one(ref, sem):
        some = ref.at[pl.ds(0, ref.shape[0] - 1)]
        pltpu.make_async_copy(some, some, sem).wait()

    def total_of(h):
        all_but_one(rparts.at[h], rs_recv.at[h])
        total = (lent_acc if h else acc)[me_r]
        for d in range(1, rows):
            total = total + rparts[h, lax.rem(me_r + d, rows)].astype(jnp.float32)
        part_f[...] = total.T
        by_set = [part_f[pl.ds(s, t_here, stride=sets), :] for s in range(sets)]
        turned = jnp.concatenate(by_set, axis=0).astype(jnp.bfloat16)
        sb[h] = turned.reshape(sb.shape[1:])

    total_of(0)

    @pl.when(is_mid)
    def _():
        total_of(1)

    def trade1(peer, slot, h):
        return pltpu.make_async_remote_copy(
            src_ref=sb.at[h, peer - 2], dst_ref=rb.at[h, slot],
            send_sem=small_send.at[(2, 5)[h]], recv_sem=trade_recv.at[(0, 2)[h]],
            device_id=(me_r, peer), device_id_type=MESH,
        )

    def trade2(peer, slot):
        return pltpu.make_async_remote_copy(
            src_ref=ob.at[peer], dst_ref=crow.at[me_r, slot - 2], send_sem=small_send.at[3], recv_sem=trade_recv.at[1],
            device_id=(me_r, peer), device_id_type=MESH,
        )

    def share(peer, slot):
        return pltpu.make_async_remote_copy(
            src_ref=crow.at[me_r], dst_ref=crow.at[slot], send_sem=small_send.at[4], recv_sem=ag_recv.at[slot],
            device_id=(peer, me_c), device_id_type=MESH,
        )

    col_peers = [lax.rem(me_c + d, cols) for d in range(1, cols)]
    row_peers = [lax.rem(me_r + d, rows) for d in range(1, rows)]
    for p in range(2, cols - 2):

        @pl.when(p != me_c)
        def _():
            trade1(p, me_c, 0).start()

            @pl.when(is_mid)
            def _():
                trade1(p, me_c, 1).start()

    exchange_time(1)
    exchange_time(2)
    for copy in small:
        copy.wait()
    product = kin[pl.ds(me_r, 1), :] * jnp.broadcast_to(trait[...], (LANES, traits)).T
    weight = product / (product + 1.0)
    s_here = sets // (cols - 4)

    def gathered(s):
        at = slice(s * t_here, (s + 1) * t_here)
        terms = []
        for c in range(cols):
            term = rb[0, c, at, :].astype(jnp.float32)
            if c // 2 in (0, lines - 1):
                term = term + rb[1, c + 2 if c // 2 == 0 else c - 2, at, :].astype(jnp.float32)
            terms.append(term)
        return jnp.concatenate(terms, axis=0)

    @pl.when(is_mid)
    def _():
        for h in range(2):
            rb[h, me_c] = sb[h, me_c - 2]
        all_but_one(rb.at[0], trade_recv.at[0])
        some = rb.at[1, pl.ds(0, cols - 5)]
        pltpu.make_async_copy(some, some, trade_recv.at[2]).wait()
        got = jnp.concatenate([gathered(s) for s in range(s_here)], axis=1)
        rotated = jnp.dot(basis[...].T, got, precision=HIGH, preferred_element_type=jnp.float32)
        scaled = rotated * jnp.concatenate([weight] * s_here, axis=1)
        back = jnp.dot(basis[...], scaled, precision=HIGH, preferred_element_type=jnp.float32)
        for s in range(s_here):
            ob[:, s * t_here:(s + 1) * t_here, :] = (
                back[:, s * LANES:(s + 1) * LANES].reshape(cols, t_here, LANES).astype(jnp.bfloat16)
            )
        for p in col_peers:
            trade2(p, me_c).start()
        crow[me_r, me_c - 2] = ob[me_c]

    exchange_time(3)
    def blocks_done(ref, sem, when_end, when_mid):
        for role, amount in ((is_end, when_end), (is_mid, when_mid)):

            @pl.when(role)
            def _():
                some = ref.at[pl.ds(0, amount)]
                pltpu.make_async_copy(some, some, sem).wait()

    blocks_done(ob, trade_recv.at[1], cols - 4, cols - 5)
    for p in row_peers:
        share(p, me_r).start()

    def place(r):
        for s in range(sets):
            part_s = crow[r, s // s_here, (s % s_here) * t_here:(s % s_here + 1) * t_here, :]
            ct[pl.ds(s, t_here, stride=sets), :] = part_s.astype(jnp.float32)
        c_out[pl.ds(pl.multiple_of(r * LANES, LANES), LANES), :] = ct[...].T.astype(jnp.bfloat16)

    place(me_r)
    exchange_time(4)
    for p in row_peers:
        share(p, p).wait_recv()
        place(p)
    size = people // TILES
    for i in range(held.shape[0] // size):
        held[i * size:(i + 1) * size, :] = tile_of(w_out, c_out, i * size, size)
    exchange_time(5)

    def count(sent, others, late):
        counts = [others + late * piece_of_unit, 0]
        for way, *_ in sent:
            counts[bank(way)] += 1
        return counts

    piece_of_unit = late / (UNITS * piece)

    @pl.when(is_end)
    def _():
        sends_done(count(end_sent, PIECES, len(late_sent["end"])))

    @pl.when(is_mid)
    def _():
        sends_done(count(mid_sent, 0, len(late_sent["mid"])))
        all_but_one(part.at[1], small_send.at[1])
        all_but_one(sb.at[1], small_send.at[5])
        all_but_one(ob, small_send.at[3])

    all_but_one(part.at[0], small_send.at[0])
    blocks_done(sb.at[0], small_send.at[2], cols - 4, cols - 5)
    all_but_one(crow, small_send.at[4])


def tile_of(w, c, first, size):
    return jnp.dot(w[first:first + size, :], c[...], preferred_element_type=jnp.float32).astype(jnp.bfloat16)


def predict(w, c, ready, gen_out, coeffs_out, held, coeffs, gen_sem):
    share = coeffs.shape[0]
    size = w.shape[0] // TILES
    done = ready.shape[0]
    copies = [pltpu.make_async_copy(ready, gen_out.at[pl.ds(0, done)], gen_sem.at[0])]
    copies[0].start()
    for i in range(done // size, TILES):
        at = pl.ds(i * size, size)
        held[at, :] = tile_of(w, c, i * size, size)
        copies.append(pltpu.make_async_copy(held.at[at], gen_out.at[at], gen_sem.at[i]))
        copies[-1].start()
        if i == done // size:
            mine = pl.ds(pl.multiple_of(lax.axis_index("row") * share, share), share)
            coeffs[...] = c[mine, :].astype(jnp.float32)
            copies.append(pltpu.make_async_copy(coeffs, coeffs_out, gen_sem.at[TILES]))
            copies[-1].start()
    for copy in copies:
        copy.wait()


def fused(panel, pheno, kin_values, trait_values, trait_basis):
    rows, cols = lax.axis_size("row"), lax.axis_size("col")
    ind, columns = pheno.shape
    traits = trait_basis.shape[0]
    sets = columns * cols // traits
    share = kin_values.shape[0] // rows
    bf, f32 = jnp.bfloat16, jnp.float32
    hbm = pl.BlockSpec(memory_space=pltpu.HBM)
    vmem = pl.BlockSpec(memory_space=pltpu.VMEM)
    dma = pltpu.SemaphoreType.DMA
    given = (panel.T, pheno, trait_basis, kin_values.reshape(rows, share), trait_values[None, :])
    whole, low, ready = pl.pallas_call(
        functools.partial(gather_rotate, rows, cols),
        out_shape=(
            pltpu.VMEM((ind, rows * share), bf),
            pltpu.VMEM((rows * share, columns), bf),
            pltpu.VMEM((ind * AHEAD // TILES, columns), bf),
        ),
        in_specs=[hbm] * 5,
        out_specs=(vmem, vmem, vmem),
        scratch_shapes=[
            pltpu.VMEM((traits, traits), f32),
            pltpu.VMEM((rows, share), f32),
            pltpu.VMEM((1, traits), f32),
            pltpu.VMEM((cols, panel.shape[1], ind), bf),
            pltpu.VMEM((ind, columns), bf),
            pltpu.VMEM((ind * len(LATE) // PIECES, columns), bf),
            pltpu.VMEM((rows, share, columns), f32),
            pltpu.VMEM((rows, share, columns), f32),
            pltpu.VMEM((columns, LANES), f32),
            pltpu.VMEM((2, rows, share, columns), bf),
            pltpu.VMEM((2, rows, share, columns), bf),
            pltpu.VMEM((2, cols - 4, columns // (cols - 4), LANES), bf),
            pltpu.VMEM((2, cols, columns // (cols - 4), LANES), bf),
            pltpu.VMEM((cols, columns // (cols - 4), LANES), bf),
            pltpu.VMEM((rows, cols - 4, columns // (cols - 4), LANES), bf),
            pltpu.VMEM((columns, LANES), f32),
            dma((5,)), dma((2,)), dma((cols, len(EARLY) + UNITS)), dma((len(LATE),)), dma((6,)), dma((2,)), dma((3,)), dma((rows,)),
        ],
        compiler_params=pltpu.CompilerParams(
            collective_id=0, has_side_effects=True, vmem_limit_bytes=36 * 1024 * 1024
        ),
    )(*(pltpu.with_memory_space_constraint(a, pltpu.HBM) for a in given))
    genetic, coeffs = pl.pallas_call(
        predict,
        out_shape=(
            jax.ShapeDtypeStruct((ind, columns), bf),
            jax.ShapeDtypeStruct((share, columns), f32),
        ),
        in_specs=[vmem] * 3,
        out_specs=(hbm, hbm),
        scratch_shapes=[pltpu.VMEM((ind, columns), bf), pltpu.VMEM((share, columns), f32), dma((TILES + 1,))],
        compiler_params=pltpu.CompilerParams(vmem_limit_bytes=20 * 1024 * 1024),
    )(whole, low, ready)
    return coeffs, genetic


def local(panel, pheno, kin_values, trait_values, trait_basis):
    rows, cols = lax.axis_size("row"), lax.axis_size("col")
    eigen = kin_values.shape[0]
    fits = 2 * panel.shape[1] == LANES and eigen // rows == LANES and trait_basis.shape[0] // cols == 16
    if fits and rows == 4 and cols == 2 * rows:
        return fused(panel, pheno, kin_values, trait_values, trait_basis)
    return plain(panel, pheno, kin_values, trait_values, trait_basis)


def plain(panel, pheno, kin_values, trait_values, trait_basis):
    col_count = lax.axis_size("col")
    columns = pheno.shape[1]
    traits = trait_basis.shape[0]
    traits_here = traits // col_count
    set_count = columns // traits_here
    sets_dev = set_count // col_count
    whole_panel = lax.all_gather(panel, "col", axis=1, tiled=True)
    partial_value = lax.dot_general(
        whole_panel, pheno, (((0,), (0,)), ((), ())), preferred_element_type=jnp.float32
    )
    summed = lax.psum_scatter(partial_value, "row", scatter_dimension=0, tiled=True)
    first_row = lax.axis_index("row") * summed.shape[0]
    share_rows = summed.shape[0]
    by_trait = summed.reshape(share_rows, traits_here, set_count).transpose(0, 2, 1)
    by_trait = by_trait.reshape(share_rows, set_count * traits_here)
    grouped = lax.all_to_all(by_trait, "col", split_axis=1, concat_axis=1, tiled=True)
    grouped = grouped.reshape(share_rows, col_count, sets_dev, traits_here).transpose(0, 2, 1, 3)
    grouped = grouped.reshape(share_rows, sets_dev, traits)
    rotated = jnp.einsum("rst,tj->rsj", grouped, trait_basis, precision=HIGH)
    kin_rows = lax.dynamic_slice_in_dim(kin_values, first_row, share_rows, 0)
    product = kin_rows[:, None] * trait_values[None, :]
    scaled = rotated * (product / (product + 1.0))[:, None, :]
    unrotated = jnp.einsum("rsj,tj->rst", scaled, trait_basis, precision=HIGH)
    outgoing = unrotated.reshape(share_rows, sets_dev, col_count, traits_here).transpose(0, 2, 1, 3)
    outgoing = outgoing.reshape(share_rows, col_count * sets_dev * traits_here)
    returned = lax.all_to_all(outgoing, "col", split_axis=1, concat_axis=1, tiled=True)
    coeffs = returned.reshape(share_rows, set_count, traits_here).transpose(0, 2, 1)
    coeffs = coeffs.reshape(share_rows, columns)
    coeffs_low = lax.all_gather(coeffs.astype(jnp.bfloat16), "row", axis=0, tiled=True)
    genetic = jnp.dot(whole_panel, coeffs_low, preferred_element_type=jnp.float32)
    return (coeffs, genetic.astype(jnp.bfloat16))


def solution(mesh):
    return jax.shard_map(
        local,
        mesh=mesh,
        in_specs=(P("row", "col"), P("row", "col"), P(), P(), P()),
        out_specs=(P("row", "col"), P("row", "col")),
        check_vma=False,
    )
```

```python
import functools

import jax
import jax.numpy as jnp
from jax import lax
from jax.experimental import pallas as pl
from jax.experimental.pallas import tpu as pltpu
from jax.sharding import PartitionSpec as P

LANES = 128
PIECES = 8
EARLY = (0, 1, 2, 3, 4, 5)
LATE = (6, 7)
FROM_END = (1, 2, 3, 4, 5)
MID_FEED = 2
UNITS = 4
END_STEPS = (
    ("P10", "P11"),
    ("P20", "T00", "P21", "T01"),
    ("P22", "T02", "P23"),
    ("P30", "T03", "P31", "P32", "T10", "T11", "T20"),
    ("P33", "T21", "T22", "T23", "T30", "T31"),
    ("T32", "T33", "B12", "B13"),
)
MID_STEPS = (
    ("O10", "O11", "O20", "O21", "O22"),
    ("O23", "O30"),
    ("O31", "O32"),
    ("O33", "O12", "O13"),
    ("X12", "X13"),
    (),
)
TILES = 16
AHEAD = 7
MESH = pl.DeviceIdType.MESH
HIGH = lax.Precision.HIGHEST


def gather_rotate(
    rows, cols, q, pheno, basis_in, kin_in, trait_in,
    w_out, c_out, held,
    basis, kin, trait, g, ph, lent, acc, lent_acc, part_f, part, rparts, sb, rb, ob, crow, ct,
    load_sem, bulk_send, recv_sem, lend_recv, small_send, rs_recv, trade_recv, ag_recv,
):
    me_r, me_c = lax.axis_index("row"), lax.axis_index("col")
    lines = cols // 2
    z, y = me_c // 2, lax.rem(me_c, 2)
    width, people = q.shape
    piece = people // PIECES
    columns = pheno.shape[1]
    traits = basis.shape[0]
    sets = columns * cols // traits
    t_here = traits // cols
    late = people * len(LATE) // PIECES
    lot = late // PIECES

    own_load = pltpu.make_async_copy(q, g.at[me_c], load_sem.at[0])
    own_load.start()
    ph_load = pltpu.make_async_copy(pheno, ph, load_sem.at[1])
    ph_load.start()
    small = [
        pltpu.make_async_copy(a, b, load_sem.at[2 + i])
        for i, (a, b) in enumerate(((basis_in, basis), (kin_in, kin), (trait_in, trait)))
    ]
    for copy in small:
        copy.start()

    far = z // (lines // 2)
    place_of = lambda k: k + far * (lines - 1 - 2 * k)
    is_end = z == place_of(0)
    is_mid = jnp.logical_not(is_end)
    own = lambda k: 2 * place_of(k) + y

    barrier = pltpu.get_barrier_semaphore()

    def greet(r, c):
        pl.semaphore_signal(barrier, inc=1, device_id=(r, c), device_id_type=MESH)

    for d in range(1, rows):
        greet(lax.rem(me_r + d, rows), me_c)
    greet(me_r, me_c + 1 - 2 * y)

    @pl.when(is_end)
    def _():
        greet(me_r, own(1))
        pl.semaphore_wait(barrier, rows + 1)

    @pl.when(is_mid)
    def _():
        greet(me_r, own(0))
        greet(me_r, own(2))
        pl.semaphore_wait(barrier, rows + 2)

    across = lambda k: 2 * place_of(k) + 1 - y
    SAME, OTHER = own, across


    def bank(way):
        return 0 if way in (0, 1) else 1

    def sends_done(counts):
        for i, count in enumerate(counts):
            rows_of = w_out.at[pl.ds(0, int(count * width * piece) // w_out.shape[1])]
            pltpu.make_async_copy(rows_of, rows_of, bulk_send.at[i]).wait()

    def hop(way, kind, k, j):
        block = kind(k)
        target = me_c + 1 - 2 * y if way == "y" else own(way)
        here = g.at[block, :, pl.ds(j * piece, piece)]
        return pltpu.make_async_remote_copy(
            src_ref=here, dst_ref=here,
            send_sem=bulk_send.at[bank(way)], recv_sem=recv_sem.at[block, j],
            device_id=(me_r, target), device_id_type=MESH,
        )

    def lend(i):
        return pltpu.make_async_remote_copy(
            src_ref=pheno.at[pl.ds(people - late + i * lot, lot)], dst_ref=lent.at[pl.ds(i * lot, lot)],
            send_sem=bulk_send.at[0], recv_sem=lend_recv.at[i * len(LATE) // PIECES],
            device_id=(me_r, own(1)), device_id_type=MESH,
        )

    def lent_here(i):
        there = lent.at[pl.ds(i * piece, piece)]
        pltpu.make_async_copy(there, there, lend_recv.at[i]).wait()

    def sender(role):
        def send(way, kind, k, j):
            role.append((way, kind, k, j))
            hop(way, kind, k, j).start()

        return send

    def arrived(kind, k, j):
        hop("y", kind, k, j).wait_recv()

    def lhs_of(k, at):
        pair = place_of(k)
        return pair, at, jnp.concatenate([g[2 * pair, :, at], g[2 * pair + 1, :, at]], axis=0)

    def turn(pair, at, lhs):
        w_out[at, pl.ds(pl.multiple_of(pair * LANES, LANES), LANES)] = lhs.T

    def process(k, j):
        pair, at, lhs = lhs_of(k, pl.ds(j * piece, piece))
        acc[pair] += jnp.dot(lhs, ph[at, :], preferred_element_type=jnp.float32)
        turn(pair, at, lhs)

    def process_lent(k, j):
        pair, _, lhs = lhs_of(k, pl.ds(j * piece, piece))
        theirs = lent[pl.ds((j - LATE[0]) * piece, piece), :]
        lent_acc[pair] += jnp.dot(lhs, theirs, preferred_element_type=jnp.float32)

    def reduce_copy(pair, h):
        return pltpu.make_async_remote_copy(
            src_ref=part.at[h, pair], dst_ref=rparts.at[h, me_r],
            send_sem=small_send.at[h], recv_sem=rs_recv.at[h],
            device_id=(pair, me_c), device_id_type=MESH,
        )

    def finish_pair(k, h=0):
        pair = place_of(k)

        @pl.when(pair != me_r)
        def _():
            part[h, pair] = (lent_acc if h else acc)[pair].astype(jnp.bfloat16)
            reduce_copy(pair, h).start()

    def unit(u):
        size = late // UNITS
        return pl.ds(people - late + u * size, size)

    def late_hop(way, kind, k, u):
        block = kind(k)
        here = g.at[block, :, unit(u)]
        return pltpu.make_async_remote_copy(
            src_ref=here, dst_ref=here, send_sem=bulk_send.at[0], recv_sem=recv_sem.at[block, len(EARLY) + u],
            device_id=(me_r, me_c + 1 - 2 * y if way == "y" else own(way)), device_id_type=MESH,
        )

    late_sent = {"end": [], "mid": []}

    def late_send_off(role, way, kind, k, u):
        late_sent[role].append((way, kind, k, u))
        late_hop(way, kind, k, u).start()

    def late_steps(role, i):
        for what, k, u in (END_STEPS if role == "end" else MID_STEPS)[i]:
            k, u = int(k), int(u)
            if what == "P":
                late_hop("y", SAME, k, u).wait_recv()
                late_send_off(role, "y", SAME, k, u)
            elif what in "OX":
                late_send_off(role, 0, SAME if what == "O" else OTHER, k, u)
            else:
                if what == "B":
                    late_hop("y", SAME, k, u).wait_recv()
                late_hop("y", OTHER, k, u).wait_recv()
                turn(*lhs_of(k, unit(u)))

    acc[...] = jnp.zeros_like(acc)
    own_load.wait()
    end_sent, mid_sent = [], []

    @pl.when(is_end)
    def _():
        send = sender(end_sent)
        for j in range(PIECES):
            send(1, SAME, 0, j)
            if j in EARLY:
                send("y", SAME, 0, j)
        for i in range(PIECES):
            lend(i).start()
        ph_load.wait()
        n = len(EARLY)
        h = n // 2
        for t in range(3 * n):
            line, j = t // n, t % n
            arrived(SAME, 1 + line, j)
            if line or j < h:
                send("y", SAME, 1 + line, j)
            if line == 0:
                arrived(OTHER, 0, j)
                if j in FROM_END:
                    send(1, OTHER, 0, j)
                process(0, j)
            elif t < n + h:
                arrived(OTHER, 1, j)
                process(1, j)
            elif t < 2 * n + h:
                arrived(OTHER, 2, t - n - h)
                process(2, t - n - h)
            else:
                arrived(OTHER, 3, t - 2 * n - h)
                process(3, t - 2 * n - h)
            if t == n - 1:
                finish_pair(0)
            if t == 2 * n + h - 1:
                finish_pair(2)
        for u in range(UNITS):
            late_send_off("end", "y", SAME, 0, u)
        for j in range(h, n):
            arrived(OTHER, 1, j)
            process(1, j)
            if j == n - 1:
                finish_pair(1)
            arrived(OTHER, 3, j)
            process(3, j)
        finish_pair(3)
        late_steps("end", 0)

    @pl.when(is_mid)
    def _():
        send = sender(mid_sent)
        n = len(EARLY)
        for j in range(PIECES):
            if j in EARLY:
                send(0, SAME, 1, j)
                send(2, SAME, 1, j)
            send("y", SAME, 1, j)
        lent_acc[...] = jnp.zeros_like(lent_acc)
        ph_load.wait()
        for j in range(PIECES):
            arrived(SAME, 0, j)
            if j in EARLY:
                send(2, SAME, 0, j)
            if j not in FROM_END:
                send("y", SAME, 0, j)
            if j in EARLY:
                arrived(SAME, 2, j)
                send(0, SAME, 2, j)
                if j not in FROM_END:
                    send("y", SAME, 2, j)
            if j == n - 1:
                for i in LATE:
                    send(2, SAME, 1, i)
            if j in LATE:
                send(2, SAME, 0, j)
                arrived(SAME, 3, j - n)
                send(0, SAME, 3, j - n)
                send("y", SAME, 3, j - n)
            arrived(OTHER, 1, j)
            process(1, j)
        for j in FROM_END:
            send(2, OTHER, 1, j)
        finish_pair(1)
        first = [j for j in range(PIECES) if j not in FROM_END]
        b = len(LATE)
        early_y = EARLY[: n // 2]
        for i, (k, j) in enumerate([(0, first[0]), (2, first[0]), (0, LATE[0]), (3, early_y[0])]):
            arrived(SAME, 3, b + i)
            send(0, SAME, 3, b + i)
            if b + i in early_y:
                send("y", SAME, 3, b + i)
            arrived(OTHER, k, j)
            process(k, j)
        for j in EARLY[n // 2:]:
            send(0, OTHER, 1, j)
        lent_here(0)
        for k in (0, 1):
            process_lent(k, LATE[0])
        here = [(2, j) for j in LATE] + [(3, j) for j in LATE]
        for (k, j), (m, i) in zip(here, [(0, LATE[1]), (3, early_y[1]), (3, early_y[2]), (2, LATE[0])]):
            arrived(SAME, k, j)
            send("y", SAME, k, j)
            arrived(OTHER, m, i)
            process(m, i)
        for j in EARLY[n // 2:]:
            send("y", SAME, 3, j)
        lent_here(1)
        for k in (0, 1):
            process_lent(k, LATE[1])
            finish_pair(k, 1)
        process_lent(2, LATE[0])
        rest = [(2, LATE[1]), (3, LATE[0]), (3, LATE[1])] + [(3, j) for j in EARLY[n // 2:]]
        for i, j in enumerate(FROM_END):
            arrived(OTHER, 0, j)
            process(0, j)
            arrived(OTHER, 2, j)
            process(2, j)
            k, m = rest.pop(0)
            arrived(OTHER, k, m)
            process(k, m)
            if m in LATE:
                process_lent(k, m)
            if m == LATE[1]:
                finish_pair(k, 1)
            if i == MID_FEED:
                late_steps("mid", 0)
        finish_pair(0)
        finish_pair(2)
        for k, m in rest:
            arrived(OTHER, k, m)
            process(k, m)
        finish_pair(3)

    def exchange_time(i):
        @pl.when(is_end)
        def _():
            late_steps("end", i)

        @pl.when(is_mid)
        def _():
            late_steps("mid", i)

    def all_but_one(ref, sem):
        some = ref.at[pl.ds(0, ref.shape[0] - 1)]
        pltpu.make_async_copy(some, some, sem).wait()

    def total_of(h):
        all_but_one(rparts.at[h], rs_recv.at[h])
        total = (lent_acc if h else acc)[me_r]
        for d in range(1, rows):
            total = total + rparts[h, lax.rem(me_r + d, rows)].astype(jnp.float32)
        part_f[...] = total.T
        by_set = [part_f[pl.ds(s, t_here, stride=sets), :] for s in range(sets)]
        turned = jnp.concatenate(by_set, axis=0).astype(jnp.bfloat16)
        sb[h] = turned.reshape(sb.shape[1:])

    total_of(0)

    @pl.when(is_mid)
    def _():
        total_of(1)

    def trade1(peer, slot, h):
        return pltpu.make_async_remote_copy(
            src_ref=sb.at[h, peer - 2], dst_ref=rb.at[h, slot],
            send_sem=small_send.at[(2, 5)[h]], recv_sem=trade_recv.at[(0, 2)[h]],
            device_id=(me_r, peer), device_id_type=MESH,
        )

    def trade2(peer, slot):
        return pltpu.make_async_remote_copy(
            src_ref=ob.at[peer], dst_ref=crow.at[me_r, slot - 2], send_sem=small_send.at[3], recv_sem=trade_recv.at[1],
            device_id=(me_r, peer), device_id_type=MESH,
        )

    def share(peer, slot):
        return pltpu.make_async_remote_copy(
            src_ref=crow.at[me_r], dst_ref=crow.at[slot], send_sem=small_send.at[4], recv_sem=ag_recv.at[slot],
            device_id=(peer, me_c), device_id_type=MESH,
        )

    col_peers = [lax.rem(me_c + d, cols) for d in range(1, cols)]
    row_peers = [lax.rem(me_r + d, rows) for d in range(1, rows)]
    for p in range(2, cols - 2):

        @pl.when(p != me_c)
        def _():
            trade1(p, me_c, 0).start()

            @pl.when(is_mid)
            def _():
                trade1(p, me_c, 1).start()

    exchange_time(1)
    exchange_time(2)
    for copy in small:
        copy.wait()
    product = kin[pl.ds(me_r, 1), :] * jnp.broadcast_to(trait[...], (LANES, traits)).T
    weight = product / (product + 1.0)
    s_here = sets // (cols - 4)

    def gathered(s):
        at = slice(s * t_here, (s + 1) * t_here)
        terms = []
        for c in range(cols):
            term = rb[0, c, at, :].astype(jnp.float32)
            if c // 2 in (0, lines - 1):
                term = term + rb[1, c + 2 if c // 2 == 0 else c - 2, at, :].astype(jnp.float32)
            terms.append(term)
        return jnp.concatenate(terms, axis=0)

    @pl.when(is_mid)
    def _():
        for h in range(2):
            rb[h, me_c] = sb[h, me_c - 2]
        all_but_one(rb.at[0], trade_recv.at[0])
        some = rb.at[1, pl.ds(0, cols - 5)]
        pltpu.make_async_copy(some, some, trade_recv.at[2]).wait()
        got = jnp.concatenate([gathered(s) for s in range(s_here)], axis=1)
        rotated = jnp.dot(basis[...].T, got, precision=HIGH, preferred_element_type=jnp.float32)
        scaled = rotated * jnp.concatenate([weight] * s_here, axis=1)
        back = jnp.dot(basis[...], scaled, precision=HIGH, preferred_element_type=jnp.float32)
        for s in range(s_here):
            ob[:, s * t_here:(s + 1) * t_here, :] = (
                back[:, s * LANES:(s + 1) * LANES].reshape(cols, t_here, LANES).astype(jnp.bfloat16)
            )
        for p in col_peers:
            trade2(p, me_c).start()
        crow[me_r, me_c - 2] = ob[me_c]

    exchange_time(3)
    def blocks_done(ref, sem, when_end, when_mid):
        for role, amount in ((is_end, when_end), (is_mid, when_mid)):

            @pl.when(role)
            def _():
                some = ref.at[pl.ds(0, amount)]
                pltpu.make_async_copy(some, some, sem).wait()

    blocks_done(ob, trade_recv.at[1], cols - 4, cols - 5)
    for p in row_peers:
        share(p, me_r).start()

    def place(r):
        for s in range(sets):
            part_s = crow[r, s // s_here, (s % s_here) * t_here:(s % s_here + 1) * t_here, :]
            ct[pl.ds(s, t_here, stride=sets), :] = part_s.astype(jnp.float32)
        c_out[pl.ds(pl.multiple_of(r * LANES, LANES), LANES), :] = ct[...].T.astype(jnp.bfloat16)

    place(me_r)
    exchange_time(4)
    for p in row_peers:
        share(p, p).wait_recv()
        place(p)
    size = people // TILES
    for i in range(held.shape[0] // size):
        held[i * size:(i + 1) * size, :] = tile_of(w_out, c_out, i * size, size)
    exchange_time(5)

    def count(sent, others, late):
        counts = [others + late * piece_of_unit, 0]
        for way, *_ in sent:
            counts[bank(way)] += 1
        return counts

    piece_of_unit = late / (UNITS * piece)

    @pl.when(is_end)
    def _():
        sends_done(count(end_sent, PIECES, len(late_sent["end"])))

    @pl.when(is_mid)
    def _():
        sends_done(count(mid_sent, 0, len(late_sent["mid"])))
        all_but_one(part.at[1], small_send.at[1])
        all_but_one(sb.at[1], small_send.at[5])
        all_but_one(ob, small_send.at[3])

    all_but_one(part.at[0], small_send.at[0])
    blocks_done(sb.at[0], small_send.at[2], cols - 4, cols - 5)
    all_but_one(crow, small_send.at[4])


def tile_of(w, c, first, size):
    return jnp.dot(w[first:first + size, :], c[...], preferred_element_type=jnp.float32).astype(jnp.bfloat16)


def predict(w, c, ready, gen_out, coeffs_out, held, coeffs, gen_sem):
    share = coeffs.shape[0]
    size = w.shape[0] // TILES
    done = ready.shape[0]
    copies = [pltpu.make_async_copy(ready, gen_out.at[pl.ds(0, done)], gen_sem.at[0])]
    copies[0].start()
    for i in range(done // size, TILES):
        at = pl.ds(i * size, size)
        held[at, :] = tile_of(w, c, i * size, size)
        copies.append(pltpu.make_async_copy(held.at[at], gen_out.at[at], gen_sem.at[i]))
        copies[-1].start()
        if i == done // size:
            mine = pl.ds(pl.multiple_of(lax.axis_index("row") * share, share), share)
            coeffs[...] = c[mine, :].astype(jnp.float32)
            copies.append(pltpu.make_async_copy(coeffs, coeffs_out, gen_sem.at[TILES]))
            copies[-1].start()
    for copy in copies:
        copy.wait()


def fused(panel, pheno, kin_values, trait_values, trait_basis):
    rows, cols = lax.axis_size("row"), lax.axis_size("col")
    ind, columns = pheno.shape
    traits = trait_basis.shape[0]
    sets = columns * cols // traits
    share = kin_values.shape[0] // rows
    bf, f32 = jnp.bfloat16, jnp.float32
    hbm = pl.BlockSpec(memory_space=pltpu.HBM)
    vmem = pl.BlockSpec(memory_space=pltpu.VMEM)
    dma = pltpu.SemaphoreType.DMA
    given = (panel.T, pheno, trait_basis, kin_values.reshape(rows, share), trait_values[None, :])
    whole, low, ready = pl.pallas_call(
        functools.partial(gather_rotate, rows, cols),
        out_shape=(
            pltpu.VMEM((ind, rows * share), bf),
            pltpu.VMEM((rows * share, columns), bf),
            pltpu.VMEM((ind * AHEAD // TILES, columns), bf),
        ),
        in_specs=[hbm] * 5,
        out_specs=(vmem, vmem, vmem),
        scratch_shapes=[
            pltpu.VMEM((traits, traits), f32),
            pltpu.VMEM((rows, share), f32),
            pltpu.VMEM((1, traits), f32),
            pltpu.VMEM((cols, panel.shape[1], ind), bf),
            pltpu.VMEM((ind, columns), bf),
            pltpu.VMEM((ind * len(LATE) // PIECES, columns), bf),
            pltpu.VMEM((rows, share, columns), f32),
            pltpu.VMEM((rows, share, columns), f32),
            pltpu.VMEM((columns, LANES), f32),
            pltpu.VMEM((2, rows, share, columns), bf),
            pltpu.VMEM((2, rows, share, columns), bf),
            pltpu.VMEM((2, cols - 4, columns // (cols - 4), LANES), bf),
            pltpu.VMEM((2, cols, columns // (cols - 4), LANES), bf),
            pltpu.VMEM((cols, columns // (cols - 4), LANES), bf),
            pltpu.VMEM((rows, cols - 4, columns // (cols - 4), LANES), bf),
            pltpu.VMEM((columns, LANES), f32),
            dma((5,)), dma((2,)), dma((cols, len(EARLY) + UNITS)), dma((len(LATE),)), dma((6,)), dma((2,)), dma((3,)), dma((rows,)),
        ],
        compiler_params=pltpu.CompilerParams(
            collective_id=0, has_side_effects=True, vmem_limit_bytes=36 * 1024 * 1024
        ),
    )(*(pltpu.with_memory_space_constraint(a, pltpu.HBM) for a in given))
    genetic, coeffs = pl.pallas_call(
        predict,
        out_shape=(
            jax.ShapeDtypeStruct((ind, columns), bf),
            jax.ShapeDtypeStruct((share, columns), f32),
        ),
        in_specs=[vmem] * 3,
        out_specs=(hbm, hbm),
        scratch_shapes=[pltpu.VMEM((ind, columns), bf), pltpu.VMEM((share, columns), f32), dma((TILES + 1,))],
        compiler_params=pltpu.CompilerParams(vmem_limit_bytes=20 * 1024 * 1024),
    )(whole, low, ready)
    return coeffs, genetic


def local(panel, pheno, kin_values, trait_values, trait_basis):
    rows, cols = lax.axis_size("row"), lax.axis_size("col")
    eigen = kin_values.shape[0]
    fits = 2 * panel.shape[1] == LANES and eigen // rows == LANES and trait_basis.shape[0] // cols == 16
    if fits and rows == 4 and cols == 2 * rows:
        return fused(panel, pheno, kin_values, trait_values, trait_basis)
    return plain(panel, pheno, kin_values, trait_values, trait_basis)


def plain(panel, pheno, kin_values, trait_values, trait_basis):
    col_count = lax.axis_size("col")
    columns = pheno.shape[1]
    traits = trait_basis.shape[0]
    traits_here = traits // col_count
    set_count = columns // traits_here
    sets_dev = set_count // col_count
    whole_panel = lax.all_gather(panel, "col", axis=1, tiled=True)
    partial_value = lax.dot_general(
        whole_panel, pheno, (((0,), (0,)), ((), ())), preferred_element_type=jnp.float32
    )
    summed = lax.psum_scatter(partial_value, "row", scatter_dimension=0, tiled=True)
    first_row = lax.axis_index("row") * summed.shape[0]
    share_rows = summed.shape[0]
    by_trait = summed.reshape(share_rows, traits_here, set_count).transpose(0, 2, 1)
    by_trait = by_trait.reshape(share_rows, set_count * traits_here)
    grouped = lax.all_to_all(by_trait, "col", split_axis=1, concat_axis=1, tiled=True)
    grouped = grouped.reshape(share_rows, col_count, sets_dev, traits_here).transpose(0, 2, 1, 3)
    grouped = grouped.reshape(share_rows, sets_dev, traits)
    rotated = jnp.einsum("rst,tj->rsj", grouped, trait_basis, precision=HIGH)
    kin_rows = lax.dynamic_slice_in_dim(kin_values, first_row, share_rows, 0)
    product = kin_rows[:, None] * trait_values[None, :]
    scaled = rotated * (product / (product + 1.0))[:, None, :]
    unrotated = jnp.einsum("rsj,tj->rst", scaled, trait_basis, precision=HIGH)
    outgoing = unrotated.reshape(share_rows, sets_dev, col_count, traits_here).transpose(0, 2, 1, 3)
    outgoing = outgoing.reshape(share_rows, col_count * sets_dev * traits_here)
    returned = lax.all_to_all(outgoing, "col", split_axis=1, concat_axis=1, tiled=True)
    coeffs = returned.reshape(share_rows, set_count, traits_here).transpose(0, 2, 1)
    coeffs = coeffs.reshape(share_rows, columns)
    coeffs_low = lax.all_gather(coeffs.astype(jnp.bfloat16), "row", axis=0, tiled=True)
    genetic = jnp.dot(whole_panel, coeffs_low, preferred_element_type=jnp.float32)
    return (coeffs, genetic.astype(jnp.bfloat16))


def solution(mesh):
    return jax.shard_map(
        local,
        mesh=mesh,
        in_specs=(P("row", "col"), P("row", "col"), P(), P(), P()),
        out_specs=(P("row", "col"), P("row", "col")),
        check_vma=False,
    )
```
